32 devices in a mesh: row: 4 (over y, x), col: 8 (over z, core).
Axes of the slice: x: 2, y: 2, z: 4, core: 2. Of those that a mesh axis runs over, the one named last changes fastest.
Arguments:
- object_tiles: float32 [2, 2, 1024, 2048], P(None, None, 'row', 'col'), may hold values from -4 to 4
- probe: float32 [2, 256, 256], replicated, may hold values from -5 to 5
- phase: float32 [256, 256], replicated, may hold values from -3.140625 to 3.140625
- measured: float32 [64, 256, 256], P(('row', 'col')), may hold values from 0 to 2
- offsets: int32 [64, 2], P(('row', 'col')), may hold values from 0 to 256
- live: int32 [4, 8], P('row', 'col'), may hold values from 1 to 2, as said below
Outputs:
- object_next: float32 [2, 2, 1024, 2048], P(None, None, 'row', 'col')
- object_grad: float32 [2, 2, 1024, 2048], P(None, None, 'row', 'col')
The draws below stay inside these ranges and needn't reach their ends.
Inputs may be any that keep to these rules, and one draw needn't show every extreme that they name: `live`: every tile has at least one used slot, and some tile uses all 2; used slots come first.
All inputs are finite; a program needn't handle non-finite values.
Results may differ from the reference program's by a relative error of at most 0.0003.
Values sent between devices are 32-bit elements; how exact they have to be, the bound alone decides.
No kernel may reach another device: no remote copies, remote signals or barrier semaphores. Data moves between devices by JAX's collectives and lax.ppermute only.
A program may use at most 64 MiB of HBM per device.

```python
import math
import jax
import jax.numpy as jnp
from jax import lax

PROBE = 256
TILE = 256
P_DEV = 2
OH = 1024
OW = 2048
POSITIONS = 64
N_ROW = 4
N_COL = 8


def draw_live(key, part):
    first_key = jax.random.fold_in(key, 11)
    second_key = jax.random.fold_in(key, 23)
    counts = jax.random.randint(first_key, (N_ROW * N_COL,), 1, P_DEV + 1)
    filled_at = jax.random.randint(second_key, (), 0, N_ROW * N_COL)
    flattened = jnp.where(jnp.arange(N_ROW * N_COL) == filled_at, P_DEV, counts)
    return flattened.reshape(N_ROW, N_COL).astype(jnp.int32)


def with_ends(result, key, smallest, high):
    longest = result.shape.index(max(result.shape))
    spots = []
    for shift in (0, 1):
        where = [jax.random.randint(jax.random.fold_in(key, axis), (), 0, length) for axis, length in enumerate(result.shape)]
        where[longest] = (where[longest] + shift) % result.shape[longest]
        spots.append(tuple(where))
    return result.at[spots[0]].set(smallest).at[spots[1]].set(high)


def steps_of(own_key, dims, split, least, largest):
    loudness, own = 1.0, jax.random.fold_in(own_key, 6)
    for position, blocks in split:
        heights = jnp.exp(jax.random.uniform(jax.random.fold_in(own, position), (blocks,), jnp.float32, least / len(split), largest / len(split)))
        loudness = loudness * jnp.repeat(heights, dims[position] // blocks).reshape([-1 if axis == position else 1 for axis in range(len(dims))])
    return loudness


def scatter_about(stream_key, dims, scale, most, shards=(), kind=jnp.bfloat16):
    gain = steps_of(stream_key, dims, shards, -0.22, 0.18) if shards else 1.0
    result = jax.random.normal(stream_key, dims, jnp.float32) * scale * gain
    return jnp.minimum(jnp.maximum(result, -most), most).astype(kind)


def setup_inputs(seed: int = 0) -> dict:
    streams_of = jax.random.split(jax.random.key(seed), 7)
    object_tiles = scatter_about(streams_of[0], (2, 2, OH, OW), 0.7, 4.0, ((2, 4), (3, 8)), jnp.float32)
    probe = scatter_about(streams_of[1], (2, PROBE, PROBE), 1.0, 5.0, (), jnp.float32)
    phase = jnp.clip(jax.random.uniform(streams_of[2], (PROBE, PROBE), jnp.float32, -3.140625, 3.140625), -3.140625, 3.140625)
    measured = jnp.clip(2.0 * jax.random.uniform(streams_of[3], (POSITIONS, PROBE, PROBE), jnp.float32) ** steps_of(streams_of[3], (POSITIONS, PROBE, PROBE), ((0, 32),), -0.2, 0.2), 0.0, 2.0)
    offsets = with_ends(jax.random.randint(streams_of[4], (POSITIONS, 2), 0, TILE + 1), jax.random.fold_in(streams_of[4], 1), 0, TILE).astype(jnp.int32)
    live = draw_live(jax.random.fold_in(streams_of[6], 71), 0)
    return dict(object_tiles=object_tiles, probe=probe, phase=phase, measured=measured, offsets=offsets, live=live)


step_size = 0.5

def dft_tables(length):
    index = jnp.arange(length, dtype=jnp.int32)
    products = index[:, None] * index[None, :] % length
    angles = products.astype(jnp.float32) * (2.0 * math.pi / length)
    norming = 1.0 / math.sqrt(length)
    return (jnp.cos(angles) * norming, jnp.sin(angles) * norming)

def apply_left(matrix, values):
    return jnp.einsum('jk,bkl->bjl', matrix, values, precision=lax.Precision.HIGHEST)

def apply_right(values, matrix):
    return jnp.einsum('bjk,kl->bjl', values, matrix, precision=lax.Precision.HIGHEST)

def transform(real_part, imag_part, cosine, sine, sign):
    first_re = apply_left(cosine, real_part) + sign * apply_left(sine, imag_part)
    first_im = apply_left(cosine, imag_part) - sign * apply_left(sine, real_part)
    final_re = apply_right(first_re, cosine) + sign * apply_right(first_im, sine)
    final_im = apply_right(first_im, cosine) - sign * apply_right(first_re, sine)
    return (final_re, final_im)

def probe_loss(windows, probe, phase, measured, weight, cosine, sine):
    slice_one_re = windows[:, 0, 0]
    slice_one_im = windows[:, 0, 1]
    slice_two_re = windows[:, 1, 0]
    slice_two_im = windows[:, 1, 1]
    probe_re = probe[0][None]
    probe_im = probe[1][None]
    first_re = probe_re * slice_one_re - probe_im * slice_one_im
    first_im = probe_re * slice_one_im + probe_im * slice_one_re
    far_re, far_im = transform(first_re, first_im, cosine, sine, 1.0)
    kernel_re = jnp.cos(phase)[None]
    kernel_im = jnp.sin(phase)[None]
    moved_re = far_re * kernel_re - far_im * kernel_im
    moved_im = far_re * kernel_im + far_im * kernel_re
    near_re, near_im = transform(moved_re, moved_im, cosine, sine, -1.0)
    exit_re = near_re * slice_two_re - near_im * slice_two_im
    exit_im = near_re * slice_two_im + near_im * slice_two_re
    wave_re, wave_im = transform(exit_re, exit_im, cosine, sine, 1.0)
    misfit = wave_re * wave_re + wave_im * wave_im - measured
    return 0.25 * jnp.sum(weight[:, None, None] * misfit * misfit)

def window_grads(windows, probe, phase, measured, weight):
    cosine, sine = dft_tables(probe.shape[1])

    def local_loss(pieces):
        return probe_loss(pieces, probe, phase, measured, weight, cosine, sine)
    loss_value, pullback = jax.vjp(local_loss, windows)
    return pullback(jnp.ones_like(loss_value))[0]

def cut_windows(source, rows_at, cols_at, length):
    anchor = jnp.zeros((), jnp.int32)

    def one_window(row_at, col_at):
        return lax.dynamic_slice(source, (anchor, anchor, row_at.astype(jnp.int32), col_at.astype(jnp.int32)), (2, 2, length, length))
    return jax.vmap(one_window)(rows_at, cols_at)

def scatter_windows(running, grads, rows_at, cols_at):
    anchor = jnp.zeros((), jnp.int32)
    length = grads.shape[3]

    def accumulate(slot_id, total):
        row_at = rows_at[slot_id].astype(jnp.int32)
        col_at = cols_at[slot_id].astype(jnp.int32)
        current = lax.dynamic_slice(total, (anchor, anchor, row_at, col_at), (2, 2, length, length))
        return lax.dynamic_update_slice(total, current + grads[slot_id], (anchor, anchor, row_at, col_at))
    return lax.fori_loop(0, grads.shape[0], accumulate, running)

def reference(object_tiles, probe, phase, measured, offsets, live):
    margin = PROBE // 2
    padded = jnp.pad(object_tiles, ((0, 0), (0, 0), (margin, margin), (margin, margin)))
    counts = live.reshape(-1)
    slot_ids = jnp.arange(P_DEV, dtype=jnp.int32)

    def per_tile(running, tile_id):
        row_tile = tile_id // N_COL
        col_tile = tile_id % N_COL
        tile_offsets = lax.dynamic_slice_in_dim(offsets, tile_id * P_DEV, P_DEV, 0)
        tile_measured = lax.dynamic_slice_in_dim(measured, tile_id * P_DEV, P_DEV, 0)
        weight = (slot_ids < counts[tile_id]).astype(jnp.float32)
        rows_at = (row_tile * TILE + tile_offsets[:, 0]).astype(jnp.int32)
        cols_at = (col_tile * TILE + tile_offsets[:, 1]).astype(jnp.int32)
        windows = cut_windows(padded, rows_at, cols_at, PROBE)
        grads = window_grads(windows, probe, phase, tile_measured, weight)
        return (scatter_windows(running, grads, rows_at, cols_at), None)
    grad_pad, _ = lax.scan(per_tile, jnp.zeros(padded.shape, jnp.float32), jnp.arange(N_ROW * N_COL, dtype=jnp.int32))
    object_grad = grad_pad[:, :, margin:margin + OH, margin:margin + OW]
    object_next = object_tiles - step_size * object_grad
    return (object_next, object_grad)
```

```python
import functools
import math

import jax
import jax.numpy as jnp
import numpy as np
from jax import lax
from jax.experimental import pallas as pl
from jax.experimental.pallas import tpu as pltpu
from jax.sharding import PartitionSpec as P

step_size = 0.5


F32 = jnp.float32
BF16 = jnp.bfloat16
VMEM = pl.BlockSpec(memory_space=pltpu.VMEM)
SMEM = pl.BlockSpec(memory_space=pltpu.SMEM)
ANY = pl.BlockSpec(memory_space=pl.ANY)


def split(value):
    high = value.astype(BF16)
    return high, (value - high.astype(F32)).astype(BF16)


def dft_tables(length):
    index = np.arange(length)
    angles = (index[:, None] * index[None, :] % length) * (2.0 * math.pi / length)
    cosine, sine = (np.cos(angles) / math.sqrt(length), np.sin(angles) / math.sqrt(length))
    left = np.block([[cosine, sine], [-sine, cosine]])
    tables = []
    for table in (left, left.T):
        high = table.astype(np.float32).astype(BF16)
        low = (table - high.astype(np.float64)).astype(np.float32).astype(BF16)
        tables.append(np.stack([high, low]))
    return tables


def transform(conj, load, store, tables, scratch):
    left, right = tables
    xh, xl, zh, zl = scratch
    length = xh.shape[0] // 2
    slots = xh.shape[1] // length
    order = (1, 0) if conj else (0, 1)
    for slot in range(slots):
        parts = load(slot)
        for at, part in enumerate(order):
            high, low = split(parts[part])
            rows, cols = pl.ds(at * length, length), pl.ds(slot * length, length)
            xh[rows, cols] = high
            xl[rows, cols] = low
    for at in range(2):
        rows = pl.ds(at * length, length)
        lhs = jnp.concatenate([left[0, rows, :], left[1, rows, :], left[0, rows, :]], axis=1)
        rhs = jnp.concatenate([xh[...], xh[...], xl[...]], axis=0)
        z = jnp.dot(lhs, rhs, preferred_element_type=F32)
        for slot in range(slots):
            high, low = split(z[:, slot * length : (slot + 1) * length])
            place = (pl.ds(slot * length, length), pl.ds(at * length, length))
            zh[place] = high
            zl[place] = low
    for slot in range(slots):
        rows = pl.ds(slot * length, length)
        lhs = jnp.concatenate([zh[rows, :], zl[rows, :], zh[rows, :]], axis=1)
        rhs = jnp.concatenate([right[0], right[0], right[1]], axis=0)
        y = jnp.dot(lhs, rhs, preferred_element_type=F32)
        both = (y[:, :length], y[:, length:])
        store(slot, both[order[0]], both[order[1]])


def gather_slice(which, pieces, places, ext, sems, margin):
    tile, row_even, row_odd, col_even, col_odd = pieces
    high, wide = tile.shape[2], tile.shape[3]
    inner_rows, inner_cols = pl.ds(margin, high), pl.ds(margin, wide)
    row_e, row_o, col_e, col_o = (pl.multiple_of(places[i], 128) for i in range(4))
    copies = [
        pltpu.make_async_copy(tile.at[which], ext.at[:, inner_rows, inner_cols], sems.at[0]),
        pltpu.make_async_copy(row_even, ext.at[:, pl.ds(row_e, margin), inner_cols], sems.at[1]),
        pltpu.make_async_copy(row_odd, ext.at[:, pl.ds(row_o, margin), inner_cols], sems.at[2]),
        pltpu.make_async_copy(col_even, ext.at[:, :, pl.ds(col_e, margin)], sems.at[3]),
        pltpu.make_async_copy(col_odd, ext.at[:, :, pl.ds(col_o, margin)], sems.at[4]),
    ]
    for copy in copies:
        copy.start()
    for copy in copies:
        copy.wait()


def place(offsets, slot, shape, length):
    spans, shifts = ([], [])
    for axis, tile in ((0, 8), (1, 128)):
        at = offsets[slot, axis]
        base = jnp.minimum(at // tile, (shape[axis + 1] - length) // tile - 1)
        spans.append(pl.ds(pl.multiple_of(base * tile, tile), length + tile))
        shifts.append(at - base * tile)
    return spans, shifts


def window(ext, offsets, slot, length):
    (rows, cols), (down, along) = place(offsets, slot, ext.shape, length)
    groups = length // 8
    sublane = lax.broadcasted_iota(jnp.int32, (1, 8, 1), 1) < 8 - down
    lane = lax.broadcasted_iota(jnp.int32, (1, 128), 1) < 128 - along
    parts = []
    for part in range(2):
        tall = ext[part, rows, cols].reshape(groups + 1, 8, length + 128)
        tall = pltpu.roll(tall, lax.rem(8 - down, 8), axis=1)
        flat = jnp.where(sublane, tall[:-1], tall[1:]).reshape(length, length + 128)
        turned = [
            pltpu.roll(flat[:, at : at + 128], lax.rem(128 - along, 128), axis=1)
            for at in range(0, length + 128, 128)
        ]
        pieces = [jnp.where(lane, *pair) for pair in zip(turned[:-1], turned[1:])]
        parts.append(jnp.concatenate(pieces, axis=1))
    return parts


def scatter(gext, offsets, slot, grads):
    length = grads[0].shape[0]
    (rows, cols), (down, along) = place(offsets, slot, gext.shape, length)
    groups = length // 8
    sublane = lax.broadcasted_iota(jnp.int32, (1, 8, 1), 1) >= down
    lane = lax.broadcasted_iota(jnp.int32, (1, 128), 1) >= along
    for part in range(2):
        turned = [
            pltpu.roll(grads[part][:, at : at + 128], lax.rem(along, 128), axis=1)
            for at in range(0, length, 128)
        ]
        none = jnp.zeros((length, 128), F32)
        pieces = [jnp.where(lane, *pair) for pair in zip([*turned, none], [none, *turned])]
        flat = jnp.concatenate(pieces, axis=1).reshape(groups, 8, length + 128)
        flat = pltpu.roll(flat, lax.rem(down, 8), axis=1)
        none = jnp.zeros((1, 8, length + 128), F32)
        after, before = (jnp.concatenate(pair, axis=0) for pair in ((flat, none), (none, flat)))
        tall = jnp.where(sublane, after, before).reshape(length + 8, length + 128)
        gext[part, rows, cols] += tall


def multiply(a, b):
    return a[0] * b[0] - a[1] * b[1], a[0] * b[1] + a[1] * b[0]


def multiply_conj(a, b):
    return a[0] * b[0] + a[1] * b[1], a[0] * b[1] - a[1] * b[0]


def put(ref, slot, re, im):
    ref[0, slot] = re
    ref[1, slot] = im


def near_kernel(
    margin, offsets, places, tile, row_e, row_o, col_e, col_o, probe, kernel, left, right,
    near, ext, mid, xh, xl, zh, zl, sems,
):
    scratch = (xh, xl, zh, zl)
    length = probe.shape[1]
    gather_slice(0, (tile, row_e, row_o, col_e, col_o), places, ext, sems, margin)

    def first(slot):
        return multiply(probe, window(ext, offsets, slot, length))

    def moved(slot, re, im):
        put(mid, slot, *multiply((re, im), kernel))

    transform(False, first, moved, (left, right), scratch)
    transform(
        True, lambda slot: (mid[0, slot], mid[1, slot]), functools.partial(put, near),
        (left, right), scratch,
    )


def exit_kernel(
    margin, offsets, places, live, tile, row_e, row_o, col_e, col_o, near, measured, left, right,
    g_near, gext, ext, mid, xh, xl, zh, zl, sems,
):
    scratch = (xh, xl, zh, zl)
    length = near.shape[2]
    gather_slice(1, (tile, row_e, row_o, col_e, col_o), places, ext, sems, margin)
    gext[...] = jnp.zeros(gext.shape, F32)

    def exiting(slot):
        return multiply((near[0, slot], near[1, slot]), window(ext, offsets, slot, length))

    def residual(slot, re, im):
        weight = jnp.where(slot < live[0, 0], 1.0, 0.0).astype(F32)
        factor = weight * (re * re + im * im - measured[slot])
        put(mid, slot, factor * re, factor * im)

    def back(slot, re, im):
        put(g_near, slot, *multiply_conj(window(ext, offsets, slot, length), (re, im)))
        scatter(gext, offsets, slot, multiply_conj((near[0, slot], near[1, slot]), (re, im)))

    transform(False, exiting, residual, (left, right), scratch)
    transform(True, lambda slot: (mid[0, slot], mid[1, slot]), back, (left, right), scratch)


def first_kernel(
    offsets, g_near, probe, kernel, left, right, gext, mid, xh, xl, zh, zl
):
    scratch = (xh, xl, zh, zl)
    gext[...] = jnp.zeros(gext.shape, F32)

    def moved(slot, re, im):
        put(mid, slot, *multiply_conj(kernel, (re, im)))

    def back(slot, re, im):
        scatter(gext, offsets, slot, multiply_conj(probe, (re, im)))

    transform(
        False, lambda slot: (g_near[0, slot], g_near[1, slot]), moved, (left, right), scratch
    )
    transform(True, lambda slot: (mid[0, slot], mid[1, slot]), back, (left, right), scratch)


def exchange(axis, to_even, to_odd):
    count = lax.axis_size(axis)
    results = []
    for start, value in ((0, to_even), (1, to_odd)):
        pairs = []
        for low in range(start, count - 1, 2):
            pairs += [(low, low + 1), (low + 1, low)]
        results.append(lax.ppermute(value, axis, pairs))
    return results


def strips(block, dim, width, even, inner):
    high = block.shape[dim] - width
    at_even = jnp.where(even, high, 0)
    return [
        lax.dynamic_slice_in_dim(block, at, width, axis=dim) for at in (at_even, high - at_even)
    ]


def per_device(object_tiles, probe, phase, measured, offsets, live):
    length = probe.shape[1]
    margin = length // 2
    slots = offsets.shape[0]
    high, wide = object_tiles.shape[2:]
    ext_shape = (2, high + 2 * margin, wide + 2 * margin)
    row_even = lax.axis_index("row") % 2 == 0
    col_even = lax.axis_index("col") % 2 == 0
    row_e = jnp.where(row_even, margin + high, 0).astype(jnp.int32)
    col_e = jnp.where(col_even, margin + wide, 0).astype(jnp.int32)
    places = jnp.stack([row_e, margin + high - row_e, col_e, margin + wide - col_e])
    left, right = (jnp.asarray(table) for table in dft_tables(length))
    kernel = jnp.stack([jnp.cos(phase), jnp.sin(phase)])

    halos = []
    for which in range(2):
        tile = object_tiles[which]
        from_rows = exchange("row", *strips(tile, 1, margin, row_even, True))
        low = jnp.where(row_even, from_rows[1], from_rows[0])
        top = jnp.where(row_even, from_rows[0], from_rows[1])
        tall = jnp.concatenate([low, tile, top], axis=1)
        from_cols = exchange("col", *strips(tall, 2, margin, col_even, True))
        halos.append((*from_rows, *from_cols))

    field = jax.ShapeDtypeStruct((2, slots, length, length), F32)
    ext = jax.ShapeDtypeStruct(ext_shape, F32)
    stages = [
        pltpu.VMEM((2 * length, slots * length), BF16),
        pltpu.VMEM((2 * length, slots * length), BF16),
        pltpu.VMEM((slots * length, 2 * length), BF16),
        pltpu.VMEM((slots * length, 2 * length), BF16),
    ]
    mid = pltpu.VMEM(field.shape, F32)
    sems = pltpu.SemaphoreType.DMA((5,))
    params = pltpu.CompilerParams(vmem_limit_bytes=40 * 1024 * 1024)
    near = pl.pallas_call(
        functools.partial(near_kernel, margin),
        out_shape=field,
        in_specs=[SMEM, SMEM] + [ANY] * 5 + [VMEM] * 4,
        out_specs=VMEM,
        scratch_shapes=[pltpu.VMEM(ext_shape, F32), mid, *stages, sems],
        compiler_params=params,
        name="near",
    )(offsets, places, object_tiles, *halos[0], probe, kernel, left, right)
    g_near, grad_one = pl.pallas_call(
        functools.partial(exit_kernel, margin),
        out_shape=(field, ext),
        in_specs=[SMEM, SMEM, SMEM] + [ANY] * 5 + [VMEM] * 4,
        out_specs=(VMEM, VMEM),
        scratch_shapes=[pltpu.VMEM(ext_shape, F32), mid, *stages, sems],
        compiler_params=params,
        name="exit",
    )(offsets, places, live, object_tiles, *halos[1], near, measured, left, right)
    grad_zero = pl.pallas_call(
        first_kernel,
        out_shape=ext,
        in_specs=[SMEM] + [VMEM] * 5,
        out_specs=VMEM,
        scratch_shapes=[mid, *stages],
        compiler_params=params,
        name="first",
    )(offsets, g_near, probe, kernel, left, right)

    grads = []
    for grad in (grad_zero, grad_one):
        from_cols = exchange("col", *strips(grad, 2, margin, col_even, False))
        right_side = jnp.where(col_even, from_cols[0], from_cols[1])
        left_side = jnp.where(col_even, from_cols[1], from_cols[0])
        inner = grad[:, :, margin:-margin]
        inner = inner.at[:, :, :margin].add(left_side)
        inner = inner.at[:, :, -margin:].add(right_side)
        from_rows = exchange("row", *strips(inner, 1, margin, row_even, False))
        low_side = jnp.where(row_even, from_rows[0], from_rows[1])
        top_side = jnp.where(row_even, from_rows[1], from_rows[0])
        tile = inner[:, margin:-margin]
        tile = tile.at[:, :margin].add(top_side)
        tile = tile.at[:, -margin:].add(low_side)
        grads.append(tile)
    folded = jnp.stack(grads)
    return (object_tiles - step_size * folded, folded)


def solution(mesh):
    return jax.shard_map(
        per_device,
        mesh=mesh,
        in_specs=(
            P(None, None, "row", "col"),
            P(),
            P(),
            P(("row", "col"), None, None),
            P(("row", "col"), None),
            P("row", "col"),
        ),
        out_specs=(P(None, None, "row", "col"), P(None, None, "row", "col")),
        check_vma=False,
    )
```

```python
import functools
import math

import jax
import jax.numpy as jnp
import numpy as np
from jax import lax
from jax.experimental import pallas as pl
from jax.experimental.pallas import tpu as pltpu
from jax.sharding import PartitionSpec as P


step_size = 0.5


F32 = jnp.float32
BF16 = jnp.bfloat16
VMEM = pl.BlockSpec(memory_space=pltpu.VMEM)
SMEM = pl.BlockSpec(memory_space=pltpu.SMEM)
ANY = pl.BlockSpec(memory_space=pl.ANY)


def split(value):
    high = value.astype(BF16)
    return high, (value - high.astype(F32)).astype(BF16)


def dft_table(length):
    index = np.arange(length)
    angles = (index[:, None] * index[None, :] % length) * (2.0 * math.pi / length)
    cosine, sine = (np.cos(angles) / math.sqrt(length), np.sin(angles) / math.sqrt(length))
    table = np.stack([cosine, cosine + sine, cosine - sine])
    high = table.astype(np.float32).astype(BF16)
    low = (table - high.astype(np.float64)).astype(np.float32).astype(BF16)
    return np.stack([high, low])


def spread(high, low, place, a, b):
    for form, value in enumerate((a + b, a, b)):
        high[(form, *place)], low[(form, *place)] = split(value)


def join(one, two, three):
    return one - three, one - two


def transform(conj, load, store, table, scratch):
    xh, xl, zh, zl = scratch
    length = xh.shape[1]
    slots = xh.shape[2] // length
    order = (1, 0) if conj else (0, 1)
    for slot in range(slots):
        parts = load(slot)
        cols = pl.ds(slot * length, length)
        spread(xh, xl, (slice(None), cols), parts[order[0]], parts[order[1]])
    products = []
    for form in range(3):
        lhs = jnp.concatenate([table[0, form], table[1, form], table[0, form]], axis=1)
        rhs = jnp.concatenate([xh[form], xh[form], xl[form]], axis=0)
        products.append(jnp.dot(lhs, rhs, preferred_element_type=F32))
    z = join(*products)
    for slot in range(slots):
        at = slice(slot * length, (slot + 1) * length)
        spread(zh, zl, (pl.ds(slot * length, length), slice(None)), z[0][:, at], z[1][:, at])
    for slot in range(slots):
        rows = pl.ds(slot * length, length)
        products = []
        for form in range(3):
            lhs = jnp.concatenate([zh[form, rows], zl[form, rows], zh[form, rows]], axis=1)
            rhs = jnp.concatenate([table[0, form], table[0, form], table[1, form]], axis=0)
            products.append(jnp.dot(lhs, rhs, preferred_element_type=F32))
        both = join(*products)
        store(slot, both[order[0]], both[order[1]])


def gather_slice(which, pieces, ext):
    tile, rows, sides, corners = pieces[0], pieces[1:3], pieces[3:5], pieces[5:7]
    margin = rows[0].shape[1]
    places = places_of(margin, *tile.shape[2:])
    inner_rows, inner_cols = pl.ds(margin, tile.shape[2]), pl.ds(margin, tile.shape[3])
    outer_rows, outer_cols = halves(places, 0, margin), halves(places, 2, margin)
    for part in range(2):
        ext[part, inner_rows, inner_cols] = tile[which, part]
        for k in range(2):
            ext[part, outer_rows[k], inner_cols] = rows[k][part]
            ext[part, inner_rows, outer_cols[k]] = sides[k][which, part]
            for j in range(2):
                ext[part, outer_rows[j], outer_cols[k]] = corners[k][j, part]


def places_of(margin, high, wide):
    row_at, col_at = lax.axis_index("row"), lax.axis_index("col")
    last = lax.axis_size("row") - 1
    row_e = jnp.where(row_at % 2 == 0, margin + high, 0)
    col_e = jnp.where(col_at % 2 == 0, margin + wide, 0)
    partnered = (row_at > 0) & ((row_at < last) | (last % 2 == 0))
    return row_e, margin + high - row_e, col_e, margin + wide - col_e, partnered


def halves(places, first, margin):
    return [pl.ds(pl.multiple_of(places[first + k], 128), margin) for k in range(2)]


def inner_halves(places, first, margin):
    at = [jnp.maximum(places[first + k] - 2 * margin, 0) for k in range(2)]
    return [pl.ds(pl.multiple_of(start, 128), margin) for start in at]


def hand_out(gext, corners, sides, middle):
    margin = corners[0].shape[2]
    places = places_of(margin, sides[0].shape[1], middle.shape[2])
    inner_rows, inner_cols = pl.ds(margin, sides[0].shape[1]), pl.ds(margin, middle.shape[2])
    outer_rows, outer_cols = halves(places, 0, margin), halves(places, 2, margin)
    for part in range(2):
        for k in range(2):
            for j in range(2):
                corners[k][j, part] = gext[part, outer_rows[j], outer_cols[k]]
            sides[k][part] = gext[part, inner_rows, outer_cols[k]]
        middle[part] = gext[part, :, inner_cols]


def place(slots_at, slot, shape, length):
    spans, shifts = ([], [])
    for axis, tile in ((0, 8), (1, 128)):
        at = slots_at[2 * slot + axis]
        base = jnp.minimum(at // tile, (shape[axis + 1] - length) // tile - 1)
        spans.append(pl.ds(pl.multiple_of(base * tile, tile), length + tile))
        shifts.append(at - base * tile)
    return spans, shifts


def window(ext, slots_at, slot, length):
    (rows, cols), (down, along) = place(slots_at, slot, ext.shape, length)
    groups = length // 8
    sublane = lax.broadcasted_iota(jnp.int32, (1, 8, 1), 1) < 8 - down
    lane = lax.broadcasted_iota(jnp.int32, (1, 128), 1) < 128 - along
    parts = []
    for part in range(2):
        tall = ext[part, rows, cols].reshape(groups + 1, 8, length + 128)
        tall = pltpu.roll(tall, lax.rem(8 - down, 8), axis=1)
        flat = jnp.where(sublane, tall[:-1], tall[1:]).reshape(length, length + 128)
        turned = [
            pltpu.roll(flat[:, at : at + 128], lax.rem(128 - along, 128), axis=1)
            for at in range(0, length + 128, 128)
        ]
        pieces = [jnp.where(lane, *pair) for pair in zip(turned[:-1], turned[1:])]
        parts.append(jnp.concatenate(pieces, axis=1))
    return parts


def scatter(gext, slots_at, slot, grads):
    length = grads[0].shape[0]
    (rows, cols), (down, along) = place(slots_at, slot, gext.shape, length)
    groups = length // 8
    sublane = lax.broadcasted_iota(jnp.int32, (1, 8, 1), 1) >= down
    lane = lax.broadcasted_iota(jnp.int32, (1, 128), 1) >= along
    for part in range(2):
        turned = [
            pltpu.roll(grads[part][:, at : at + 128], lax.rem(along, 128), axis=1)
            for at in range(0, length, 128)
        ]
        none = jnp.zeros((length, 128), F32)
        pieces = [jnp.where(lane, *pair) for pair in zip([*turned, none], [none, *turned])]
        flat = jnp.concatenate(pieces, axis=1).reshape(groups, 8, length + 128)
        flat = pltpu.roll(flat, lax.rem(down, 8), axis=1)
        none = jnp.zeros((1, 8, length + 128), F32)
        after, before = (jnp.concatenate(pair, axis=0) for pair in ((flat, none), (none, flat)))
        tall = jnp.where(sublane, after, before).reshape(length + 8, length + 128)
        gext[part, rows, cols] += tall


def multiply(a, b):
    return a[0] * b[0] - a[1] * b[1], a[0] * b[1] + a[1] * b[0]


def multiply_conj(a, b):
    return a[0] * b[0] + a[1] * b[1], a[0] * b[1] - a[1] * b[0]


def put(ref, slot, re, im):
    ref[0, slot] = re
    ref[1, slot] = im


def near_kernel(
    slots_at, tile, row_e, row_o, side_e, side_o, corner_e, corner_o, probe, kernel, left, near,
    ext, mid, xh, xl, zh, zl,
):
    scratch = (xh, xl, zh, zl)
    length = probe.shape[1]
    pieces = (tile, row_e, row_o, side_e, side_o, corner_e, corner_o)
    gather_slice(0, pieces, ext)

    def first(slot):
        return multiply(probe, window(ext, slots_at, slot, length))

    def moved(slot, re, im):
        put(mid, slot, *multiply((re, im), kernel))

    transform(False, first, moved, left, scratch)
    transform(
        True, lambda slot: (mid[0, slot], mid[1, slot]), functools.partial(put, near),
        left, scratch,
    )


def exit_kernel(
    slots_at, tile, row_e, row_o, side_e, side_o, corner_e, corner_o, near, measured, left,
    g_near, out_ce, out_co, out_se, out_so, middle, gext, ext, mid, cut, xh, xl,
    zh, zl,
):
    scratch = (xh, xl, zh, zl)
    length = near.shape[2]
    pieces = (tile, row_e, row_o, side_e, side_o, corner_e, corner_o)
    gather_slice(1, pieces, ext)
    gext[...] = jnp.zeros(gext.shape, F32)

    def exiting(slot):
        put(cut, slot, *window(ext, slots_at, slot, length))
        return multiply((near[0, slot], near[1, slot]), (cut[0, slot], cut[1, slot]))

    def residual(slot, re, im):
        weight = jnp.where(slot < slots_at[2 * near.shape[1]], 1.0, 0.0).astype(F32)
        factor = weight * (re * re + im * im - measured[slot])
        put(mid, slot, factor * re, factor * im)

    def back(slot, re, im):
        put(g_near, slot, *multiply_conj((cut[0, slot], cut[1, slot]), (re, im)))
        scatter(gext, slots_at, slot, multiply_conj((near[0, slot], near[1, slot]), (re, im)))

    transform(False, exiting, residual, left, scratch)
    transform(True, lambda slot: (mid[0, slot], mid[1, slot]), back, left, scratch)
    hand_out(gext, (out_ce, out_co), (out_se, out_so), middle)


def first_kernel(
    slots_at, g_near, probe, kernel, left, one_se, one_so, out_ce, out_co, out_se,
    out_so, middle, gext, mid, xh, xl, zh, zl,
):
    scratch = (xh, xl, zh, zl)
    gext[...] = jnp.zeros(gext.shape, F32)

    def moved(slot, re, im):
        put(mid, slot, *multiply_conj(kernel, (re, im)))

    def back(slot, re, im):
        scatter(gext, slots_at, slot, multiply_conj(probe, (re, im)))

    transform(
        False, lambda slot: (g_near[0, slot], g_near[1, slot]), moved, left, scratch
    )
    transform(True, lambda slot: (mid[0, slot], mid[1, slot]), back, left, scratch)
    hand_out(gext, (out_ce, out_co), (out_se.at[0], out_so.at[0]), middle)
    out_se[1] = one_se[...]
    out_so[1] = one_so[...]


def corner_kernel(middle, corner_e, corner_o, strip_e, *strips_o):
    corners, margin = (corner_e, corner_o), corner_e.shape[2]
    places = places_of(margin, middle.shape[1] - 2 * margin, middle.shape[2])
    rows, cols = halves(places, 0, margin), inner_halves(places, 2, margin)
    for part in range(2):
        for strip, at in ((strip_e.at[part], rows[0]), (half(strips_o, part), rows[1])):
            strip[...] = middle[part, at, :]
            for k in range(2):
                strip[:, cols[k]] += corners[k][int(at is rows[1]), part]
    if len(strips_o) == 2:
        relayed = strips_o[1]
        relayed[...] = jnp.where(places[4], relayed[...], 0.0)


def half(strips, part):
    return strips[part].at[0] if len(strips) == 2 else strips[0].at[part]


def final_kernel(steps, tile, side_e, side_o, *refs):
    after, grad, new_after, new_grad, sems = refs[-5:]
    margin = side_e.shape[3]
    places = places_of(margin, *tile.shape[2:])
    rows, cols = inner_halves(places, 0, margin), inner_halves(places, 2, margin)
    copies = []
    for index, (which, side, middle, arrived) in enumerate(steps):
        arrived = [refs[at] for at in arrived]
        outer = pl.ds(pl.multiple_of(rows[side].start + margin, 128), margin)
        for part in range(2):
            new = new_grad.at[index, part]
            new[...] = refs[middle][part, outer, :] + half(arrived, part)[...]
            for k in range(2):
                new[:, cols[k]] += (side_e, side_o)[k][which, part, rows[side], :]
            stepped = tile[which, part, rows[side], :] - step_size * new[...]
            new_after[index, part] = stepped
            for at, (source, out) in enumerate(((new_after, after), (new_grad, grad))):
                copy = pltpu.make_async_copy(
                    source.at[index, part], out.at[which, part, rows[side], :],
                    sems.at[index, part, at],
                )
                copy.start()
                copies.append(copy)
    for copy in copies:
        copy.wait()


def edge_kernel(tile, row_e0, row_o0, row_e1, row_o1, side_e, side_o):
    margin = row_e0.shape[1]
    places = places_of(margin, *tile.shape[2:])
    rows, cols = inner_halves(places, 0, margin), inner_halves(places, 2, margin)
    for which, outs in enumerate(((row_e0, row_o0), (row_e1, row_o1))):
        for part in range(2):
            for k in range(2):
                outs[k][part] = tile[which, part, rows[k], :]
                (side_e, side_o)[k][which, part] = tile[which, part, :, cols[k]]
    row_o1[...] = jnp.where(places[4], row_o1[...], 0.0)


def cut_kernel(halo_e, halo_o, to_even, to_odd):
    margin = to_even.shape[2]
    cols = inner_halves(places_of(margin, 0, halo_e.shape[2]), 2, margin)
    for j, halo in enumerate((halo_e, halo_o)):
        for part in range(2):
            to_even[j, part] = halo[part, :, cols[0]]
            to_odd[j, part] = halo[part, :, cols[1]]


def turn_kernel(offsets, live, phase, table, light, slots_at, kernel, left, probe):
    for slot in range(offsets.shape[0]):
        for axis in range(2):
            slots_at[2 * slot + axis] = offsets[slot, axis]
    slots_at[2 * offsets.shape[0]] = live[0, 0]
    left[...] = table[...]
    probe[...] = light[...]
    kernel[0] = jnp.cos(phase[...])
    kernel[1] = jnp.sin(phase[...])


def even_pairs(count):
    return [(low, low + 1) for low in range(0, count - 1, 2)]


def odd_pairs(count):
    return [(low, low + 1) for low in range(1, count - 1, 2)]


def swap(axis, value, odd):
    count = lax.axis_size(axis)
    pairs = odd_pairs(count) if odd else even_pairs(count)
    return lax.ppermute(value, axis, pairs + [(high, low) for low, high in pairs])


def closed(steps, spare):
    steps = list(steps)
    for source, target in spare:
        if all(source != a and target != b for a, b in steps):
            steps.append((source, target))
    return steps


def relay_steps(count, fill):
    pairs = odd_pairs(count)
    out = [(low, low + 2) for low, high in pairs] + [(high, high - 2) for low, high in pairs]
    home = [(low + 2, high) for low, high in pairs] + [(high - 2, low) for low, high in pairs]
    spares = ([(b, a) for a, b in out], out) if fill else ([], [])
    return closed(out, spares[0]), closed(home, spares[1])


def relay(axis, value, step, fill):
    count = lax.axis_size(axis)
    if count % 2 == 0:
        steps = relay_steps(count, fill)[step]
    else:
        pairs = odd_pairs(count)
        steps = [pairs + [(high, low) for low, high in pairs], [(i, i) for i in range(count)]][step]
    return lax.ppermute(value, axis, steps)


def per_device(object_tiles, probe, phase, measured, offsets, live):
    length = probe.shape[1]
    margin = length // 2
    slots = offsets.shape[0]
    high, wide = object_tiles.shape[2:]
    ext_shape = (2, high + 2 * margin, wide + 2 * margin)
    assert high == 2 * margin
    table = jnp.asarray(dft_table(length))

    def shape(*dims):
        return jax.ShapeDtypeStruct(dims, F32)

    field = shape(2, slots, length, length)
    pieces = (
        *[shape(2, 2, margin, margin)] * 2,
        *[shape(2, high, margin)] * 2,
        shape(2, high + 2 * margin, wide),
    )
    strip = shape(2, margin, wide)
    ext = pltpu.VMEM(ext_shape, F32)
    mid = pltpu.VMEM(field.shape, F32)
    stages = [
        *[pltpu.VMEM((3, length, slots * length), BF16)] * 2,
        *[pltpu.VMEM((3, slots * length, length), BF16)] * 2,
    ]
    params = pltpu.CompilerParams(vmem_limit_bytes=20 * 1024 * 1024)
    small = pltpu.CompilerParams(vmem_limit_bytes=6 * 1024 * 1024)
    cost = pl.CostEstimate(
        flops=2 * 2 * 9 * 2 * slots * length**3, bytes_accessed=8 << 20,
        transcendentals=0,
    )
    call = functools.partial(pl.pallas_call, compiler_params=params)
    call_small = functools.partial(pl.pallas_call, compiler_params=small)
    sides = shape(2, 2, high, margin)
    row_e0, row_o0, row_e1, row_o1, side_e, side_o = call_small(
        edge_kernel,
        out_shape=(*[strip] * 4, sides, sides),
        in_specs=[VMEM],
        out_specs=(VMEM,) * 6,
        name="edges",
    )(object_tiles)
    away = relay("row", row_o1, 0, True)
    halo_e0 = swap("row", row_e0, False)
    halo_o0 = swap("row", row_o0, True)
    halo_e1 = swap("row", row_e1, False)
    side_e = swap("col", side_e, False)
    side_o = swap("col", side_o, True)
    halo_o1 = relay("row", away, 1, True)
    slots_at, kernel, left, probe = call_small(
        turn_kernel,
        out_shape=(
            jax.ShapeDtypeStruct((2 * slots + 1,), jnp.int32),
            shape(2, length, length),
            jax.ShapeDtypeStruct(table.shape, BF16),
            shape(*probe.shape),
        ),
        in_specs=[SMEM] * 2 + [VMEM] * 3,
        out_specs=(SMEM, VMEM, VMEM, VMEM),
        name="turn",
    )(offsets, live, phase, table, probe)

    corners = []
    for which, halo in enumerate(((halo_e0, halo_o0), (halo_e1, halo_o1))):
        to_even, to_odd = call_small(
            cut_kernel,
            out_shape=(shape(2, 2, margin, margin),) * 2,
            in_specs=[VMEM, VMEM],
            out_specs=(VMEM, VMEM),
            name=f"cut_{which}",
        )(*halo)
        corners.append((swap("col", to_even, False), swap("col", to_odd, True)))
    near = call(
        near_kernel,
        out_shape=field,
        in_specs=[SMEM] + [VMEM] * 10,
        out_specs=VMEM,
        scratch_shapes=[ext, mid, *stages],
        cost_estimate=cost,
        name="near",
    )(
        slots_at, object_tiles, halo_e0, halo_o0, side_e, side_o, *corners[0], probe, kernel,
        left,
    )
    g_near, corner_e, corner_o, one_e, one_o, middle_one = call(
        exit_kernel,
        out_shape=(field, *pieces),
        in_specs=[SMEM] + [VMEM] * 10,
        out_specs=(VMEM,) * 6,
        scratch_shapes=[ext, ext, mid, mid, *stages],
        cost_estimate=cost,
        name="exit",
    )(
        slots_at, object_tiles, halo_e1, halo_o1, side_e, side_o, *corners[1], near,
        measured, left,
    )

    def outer_rows(name, odd, middle, corner_e, corner_o):
        return call_small(
            corner_kernel,
            out_shape=(strip, *odd),
            in_specs=[VMEM] * 3,
            out_specs=(VMEM,) * (1 + len(odd)),
            name=name,
        )(middle, corner_e, corner_o)

    corner_e = swap("col", corner_e, False)
    corner_o = swap("col", corner_o, True)
    zero_e, zero_o, side_e, side_o, middle_zero = call(
        first_kernel,
        out_shape=(*pieces[:2], sides, sides, pieces[4]),
        in_specs=[SMEM] + [VMEM] * 6,
        out_specs=(VMEM,) * 5,
        scratch_shapes=[ext, mid, *stages],
        cost_estimate=cost,
        name="first",
    )(slots_at, g_near, probe, kernel, left, one_e, one_o)
    rows_e1, rows_o1 = outer_rows("fold_one", (strip,), middle_one, corner_e, corner_o)
    rows_e1 = swap("row", rows_e1, False)
    rows_o1 = [swap("row", rows_o1, True)]
    zero_e = swap("col", zero_e, False)
    zero_o = swap("col", zero_o, True)
    rows_e0, direct, away = outer_rows(
        "fold_zero", (shape(1, margin, wide),) * 2, middle_zero, zero_e, zero_o
    )
    away = relay("row", away, 0, False)
    rows_e0 = swap("row", rows_e0, False)
    direct = swap("row", direct, True)
    rows_o0 = [direct, relay("row", away, 1, False)]
    side_e = swap("col", side_e, False)
    side_o = swap("col", side_o, True)
    whole = shape(*object_tiles.shape)
    outs = ()
    for given, steps in (
        ((middle_one, rows_e1, *rows_o1), ((1, 0, 0, [1]), (1, 1, 0, [2]))),
        ((middle_zero, rows_e0), ((0, 0, 0, [1]),)),
        ((middle_zero, *rows_o0), ((0, 1, 0, [1, 2]),)),
    ):
        rows = pltpu.VMEM((len(steps), 2, margin, wide), F32)
        outs = pl.pallas_call(
            functools.partial(final_kernel, steps),
            out_shape=(whole, whole),
            in_specs=[VMEM] * (3 + len(given)) + [ANY] * len(outs),
            out_specs=(ANY, ANY),
            scratch_shapes=[rows, rows, pltpu.SemaphoreType.DMA((len(steps), 2, 2))],
            input_output_aliases={3 + len(given): 0, 4 + len(given): 1} if outs else {},
            compiler_params=small,
        )(object_tiles, side_e, side_o, *given, *outs)
    return tuple(outs)


def solution(mesh):
    return jax.shard_map(
        per_device,
        mesh=mesh,
        in_specs=(
            P(None, None, "row", "col"),
            P(),
            P(),
            P(("row", "col"), None, None),
            P(("row", "col"), None),
            P("row", "col"),
        ),
        out_specs=(P(None, None, "row", "col"), P(None, None, "row", "col")),
        check_vma=False,
    )
```

```python
import functools
import math

import jax
import jax.numpy as jnp
import numpy as np
from jax import lax
from jax.experimental import pallas as pl
from jax.experimental.pallas import tpu as pltpu
from jax.sharding import PartitionSpec as P


step_size = 0.5


F32 = jnp.float32
BF16 = jnp.bfloat16
VMEM = pl.BlockSpec(memory_space=pltpu.VMEM)
SMEM = pl.BlockSpec(memory_space=pltpu.SMEM)
ANY = pl.BlockSpec(memory_space=pl.ANY)


def split(value):
    high = value.astype(BF16)
    return high, (value - high.astype(F32)).astype(BF16)


def dft_table(length):
    index = np.arange(length)
    angles = (index[:, None] * index[None, :] % length) * (2.0 * math.pi / length)
    cosine, sine = (np.cos(angles) / math.sqrt(length), np.sin(angles) / math.sqrt(length))
    table = np.stack([cosine, cosine + sine, cosine - sine])
    high = table.astype(np.float32).astype(BF16)
    low = (table - high.astype(np.float64)).astype(np.float32).astype(BF16)
    return np.stack([high, low])


def spread(high, low, place, a, b):
    for form, value in enumerate((a + b, a, b)):
        high[(form, *place)], low[(form, *place)] = split(value)


def join(one, two, three):
    return one - three, one - two


def transform(conj, load, store, table, scratch):
    xh, xl, zh, zl = scratch
    length = xh.shape[1]
    slots = xh.shape[2] // length
    order = (1, 0) if conj else (0, 1)
    for slot in range(slots):
        parts = load(slot)
        cols = pl.ds(slot * length, length)
        spread(xh, xl, (slice(None), cols), parts[order[0]], parts[order[1]])
    products = []
    for form in range(3):
        lhs = jnp.concatenate([table[0, form], table[1, form], table[0, form]], axis=1)
        rhs = jnp.concatenate([xh[form], xh[form], xl[form]], axis=0)
        products.append(jnp.dot(lhs, rhs, preferred_element_type=F32))
    z = join(*products)
    for slot in range(slots):
        at = slice(slot * length, (slot + 1) * length)
        spread(zh, zl, (pl.ds(slot * length, length), slice(None)), z[0][:, at], z[1][:, at])
    for slot in range(slots):
        rows = pl.ds(slot * length, length)
        products = []
        for form in range(3):
            lhs = jnp.concatenate([zh[form, rows], zl[form, rows], zh[form, rows]], axis=1)
            rhs = jnp.concatenate([table[0, form], table[0, form], table[1, form]], axis=0)
            products.append(jnp.dot(lhs, rhs, preferred_element_type=F32))
        both = join(*products)
        store(slot, both[order[0]], both[order[1]])


def gather_slice(which, pieces, ext):
    tile, rows, sides, corners = pieces[0], pieces[1:3], pieces[3:5], pieces[5:7]
    margin = rows[0].shape[1]
    places = places_of(margin, *tile.shape[2:])
    inner_rows, inner_cols = pl.ds(margin, tile.shape[2]), pl.ds(margin, tile.shape[3])
    outer_rows, outer_cols = halves(places, 0, margin), halves(places, 2, margin)
    for part in range(2):
        ext[part, inner_rows, inner_cols] = tile[which, part]
        for k in range(2):
            ext[part, outer_rows[k], inner_cols] = rows[k][part]
            ext[part, inner_rows, outer_cols[k]] = sides[k][which, part]
            for j in range(2):
                ext[part, outer_rows[j], outer_cols[k]] = corners[k][j, part]


def places_of(margin, high, wide):
    row_at, col_at = lax.axis_index("row"), lax.axis_index("col")
    last = lax.axis_size("row") - 1
    row_e = jnp.where(row_at % 2 == 0, margin + high, 0)
    col_e = jnp.where(col_at % 2 == 0, margin + wide, 0)
    partnered = (row_at > 0) & ((row_at < last) | (last % 2 == 0))
    return row_e, margin + high - row_e, col_e, margin + wide - col_e, partnered


def halves(places, first, margin):
    return [pl.ds(pl.multiple_of(places[first + k], 128), margin) for k in range(2)]


def inner_halves(places, first, margin):
    at = [jnp.maximum(places[first + k] - 2 * margin, 0) for k in range(2)]
    return [pl.ds(pl.multiple_of(start, 128), margin) for start in at]


def hand_out(gext, corners, sides, middle):
    margin = corners[0].shape[2]
    places = places_of(margin, sides[0].shape[1], middle.shape[2])
    inner_rows, inner_cols = pl.ds(margin, sides[0].shape[1]), pl.ds(margin, middle.shape[2])
    outer_rows, outer_cols = halves(places, 0, margin), halves(places, 2, margin)
    for part in range(2):
        for k in range(2):
            for j in range(2):
                corners[k][j, part] = gext[part, outer_rows[j], outer_cols[k]]
            sides[k][part] = gext[part, inner_rows, outer_cols[k]]
        middle[part] = gext[part, :, inner_cols]


def scalar(slots_at, index):
    return jnp.max(slots_at[pl.ds(index, 1), :]).astype(jnp.int32)


def place(slots_at, slot, shape, length):
    spans, shifts = ([], [])
    for axis, tile in ((0, 8), (1, 128)):
        at = scalar(slots_at, 2 * slot + axis)
        base = jnp.minimum(at // tile, (shape[axis + 1] - length) // tile - 1)
        spans.append(pl.ds(pl.multiple_of(base * tile, tile), length + tile))
        shifts.append(at - base * tile)
    return spans, shifts


def window(ext, slots_at, slot, length):
    (rows, cols), (down, along) = place(slots_at, slot, ext.shape, length)
    groups = length // 8
    sublane = lax.broadcasted_iota(jnp.int32, (1, 8, 1), 1) < 8 - down
    lane = lax.broadcasted_iota(jnp.int32, (1, 128), 1) < 128 - along
    parts = []
    for part in range(2):
        tall = ext[part, rows, cols].reshape(groups + 1, 8, length + 128)
        tall = pltpu.roll(tall, lax.rem(8 - down, 8), axis=1)
        flat = jnp.where(sublane, tall[:-1], tall[1:]).reshape(length, length + 128)
        turned = [
            pltpu.roll(flat[:, at : at + 128], lax.rem(128 - along, 128), axis=1)
            for at in range(0, length + 128, 128)
        ]
        pieces = [jnp.where(lane, *pair) for pair in zip(turned[:-1], turned[1:])]
        parts.append(jnp.concatenate(pieces, axis=1))
    return parts


def scatter(gext, slots_at, slot, grads):
    length = grads[0].shape[0]
    (rows, cols), (down, along) = place(slots_at, slot, gext.shape, length)
    groups = length // 8
    sublane = lax.broadcasted_iota(jnp.int32, (1, 8, 1), 1) >= down
    lane = lax.broadcasted_iota(jnp.int32, (1, 128), 1) >= along
    for part in range(2):
        turned = [
            pltpu.roll(grads[part][:, at : at + 128], lax.rem(along, 128), axis=1)
            for at in range(0, length, 128)
        ]
        none = jnp.zeros((length, 128), F32)
        pieces = [jnp.where(lane, *pair) for pair in zip([*turned, none], [none, *turned])]
        flat = jnp.concatenate(pieces, axis=1).reshape(groups, 8, length + 128)
        flat = pltpu.roll(flat, lax.rem(down, 8), axis=1)
        none = jnp.zeros((1, 8, length + 128), F32)
        after, before = (jnp.concatenate(pair, axis=0) for pair in ((flat, none), (none, flat)))
        tall = jnp.where(sublane, after, before).reshape(length + 8, length + 128)
        gext[part, rows, cols] += tall


def multiply(a, b):
    return a[0] * b[0] - a[1] * b[1], a[0] * b[1] + a[1] * b[0]


def multiply_conj(a, b):
    return a[0] * b[0] + a[1] * b[1], a[0] * b[1] - a[1] * b[0]


def put(ref, slot, re, im):
    ref[0, slot] = re
    ref[1, slot] = im


def near_kernel(
    slots_at, tile, row_e, row_o, side_e, side_o, corner_e, corner_o, probe, kernel, left, near,
    ext, mid, xh, xl, zh, zl,
):
    scratch = (xh, xl, zh, zl)
    length = probe.shape[1]
    pieces = (tile, row_e, row_o, side_e, side_o, corner_e, corner_o)
    gather_slice(0, pieces, ext)

    def first(slot):
        return multiply(probe, window(ext, slots_at, slot, length))

    def moved(slot, re, im):
        put(mid, slot, *multiply((re, im), kernel))

    transform(False, first, moved, left, scratch)
    transform(
        True, lambda slot: (mid[0, slot], mid[1, slot]), functools.partial(put, near),
        left, scratch,
    )


def exit_kernel(
    slots_at, tile, row_e, row_o, side_e, side_o, corner_e, corner_o, near, measured, left,
    g_near, out_ce, out_co, out_se, out_so, middle, gext, ext, mid, cut, xh, xl,
    zh, zl,
):
    scratch = (xh, xl, zh, zl)
    length = near.shape[2]
    pieces = (tile, row_e, row_o, side_e, side_o, corner_e, corner_o)
    gather_slice(1, pieces, ext)
    gext[...] = jnp.zeros(gext.shape, F32)

    def exiting(slot):
        put(cut, slot, *window(ext, slots_at, slot, length))
        return multiply((near[0, slot], near[1, slot]), (cut[0, slot], cut[1, slot]))

    def residual(slot, re, im):
        weight = jnp.where(slot < scalar(slots_at, 2 * near.shape[1]), 1.0, 0.0).astype(F32)
        factor = weight * (re * re + im * im - measured[slot])
        put(mid, slot, factor * re, factor * im)

    def back(slot, re, im):
        put(g_near, slot, *multiply_conj((cut[0, slot], cut[1, slot]), (re, im)))
        scatter(gext, slots_at, slot, multiply_conj((near[0, slot], near[1, slot]), (re, im)))

    transform(False, exiting, residual, left, scratch)
    transform(True, lambda slot: (mid[0, slot], mid[1, slot]), back, left, scratch)
    hand_out(gext, (out_ce, out_co), (out_se, out_so), middle)


def first_kernel(
    slots_at, g_near, probe, kernel, left, one_se, one_so, out_ce, out_co, out_se,
    out_so, middle, gext, mid, xh, xl, zh, zl,
):
    scratch = (xh, xl, zh, zl)
    gext[...] = jnp.zeros(gext.shape, F32)

    def moved(slot, re, im):
        put(mid, slot, *multiply_conj(kernel, (re, im)))

    def back(slot, re, im):
        scatter(gext, slots_at, slot, multiply_conj(probe, (re, im)))

    transform(
        False, lambda slot: (g_near[0, slot], g_near[1, slot]), moved, left, scratch
    )
    transform(True, lambda slot: (mid[0, slot], mid[1, slot]), back, left, scratch)
    hand_out(gext, (out_ce, out_co), (out_se.at[0], out_so.at[0]), middle)
    out_se[1] = one_se[...]
    out_so[1] = one_so[...]


def corner_kernel(middle, corner_e, corner_o, strip_e, *strips_o):
    corners, margin = (corner_e, corner_o), corner_e.shape[2]
    places = places_of(margin, middle.shape[1] - 2 * margin, middle.shape[2])
    rows, cols = halves(places, 0, margin), inner_halves(places, 2, margin)
    for part in range(2):
        for strip, at in ((strip_e.at[part], rows[0]), (half(strips_o, part), rows[1])):
            strip[...] = middle[part, at, :]
            for k in range(2):
                strip[:, cols[k]] += corners[k][int(at is rows[1]), part]
    if len(strips_o) == 2:
        relayed = strips_o[1]
        relayed[...] = jnp.where(places[4], relayed[...], 0.0)


def half(strips, part):
    return strips[part].at[0] if len(strips) == 2 else strips[0].at[part]


def final_kernel(steps, tile, side_e, side_o, *refs):
    after, grad, new_after, new_grad, sems = refs[-5:]
    margin = side_e.shape[3]
    places = places_of(margin, *tile.shape[2:])
    rows, cols = inner_halves(places, 0, margin), inner_halves(places, 2, margin)
    copies = []
    for index, (which, side, middle, arrived) in enumerate(steps):
        arrived = [refs[at] for at in arrived]
        outer = pl.ds(pl.multiple_of(rows[side].start + margin, 128), margin)
        for part in range(2):
            new = new_grad.at[index, part]
            new[...] = refs[middle][part, outer, :] + half(arrived, part)[...]
            for k in range(2):
                new[:, cols[k]] += (side_e, side_o)[k][which, part, rows[side], :]
            stepped = tile[which, part, rows[side], :] - step_size * new[...]
            new_after[index, part] = stepped
            for at, (source, out) in enumerate(((new_after, after), (new_grad, grad))):
                copy = pltpu.make_async_copy(
                    source.at[index, part], out.at[which, part, rows[side], :],
                    sems.at[index, part, at],
                )
                copy.start()
                copies.append(copy)
    for copy in copies:
        copy.wait()


def edge_kernel(tile, row_e0, row_o0, row_e1, row_o1, side_e, side_o):
    margin = row_e0.shape[1]
    places = places_of(margin, *tile.shape[2:])
    rows, cols = inner_halves(places, 0, margin), inner_halves(places, 2, margin)
    for which, outs in enumerate(((row_e0, row_o0), (row_e1, row_o1))):
        for part in range(2):
            for k in range(2):
                outs[k][part] = tile[which, part, rows[k], :]
                (side_e, side_o)[k][which, part] = tile[which, part, :, cols[k]]
    row_o1[...] = jnp.where(places[4], row_o1[...], 0.0)


def cut_kernel(halo_e, halo_o, to_even, to_odd):
    margin = to_even.shape[2]
    cols = inner_halves(places_of(margin, 0, halo_e.shape[2]), 2, margin)
    for j, halo in enumerate((halo_e, halo_o)):
        for part in range(2):
            to_even[j, part] = halo[part, :, cols[0]]
            to_odd[j, part] = halo[part, :, cols[1]]


def turn_kernel(offsets, live, phase, table, light, slots_at, kernel, left, probe):
    count = offsets.shape[0]
    scalars = [offsets[slot, axis] for slot in range(count) for axis in range(2)] + [live[0, 0]]
    row = lax.broadcasted_iota(jnp.int32, slots_at.shape, 0)
    total = jnp.zeros(slots_at.shape, jnp.int32)
    for index, scalar in enumerate(scalars):
        total = jnp.where(row == index, scalar, total)
    slots_at[...] = total.astype(F32)
    left[...] = table[...]
    probe[...] = light[...]
    kernel[0] = jnp.cos(phase[...])
    kernel[1] = jnp.sin(phase[...])


def even_pairs(count):
    return [(low, low + 1) for low in range(0, count - 1, 2)]


def odd_pairs(count):
    return [(low, low + 1) for low in range(1, count - 1, 2)]


def swap(axis, value, odd):
    count = lax.axis_size(axis)
    pairs = odd_pairs(count) if odd else even_pairs(count)
    return lax.ppermute(value, axis, pairs + [(high, low) for low, high in pairs])


def closed(steps, spare):
    steps = list(steps)
    for source, target in spare:
        if all(source != a and target != b for a, b in steps):
            steps.append((source, target))
    return steps


def relay_steps(count, fill):
    pairs = odd_pairs(count)
    out = [(low, low + 2) for low, high in pairs] + [(high, high - 2) for low, high in pairs]
    home = [(low + 2, high) for low, high in pairs] + [(high - 2, low) for low, high in pairs]
    spares = ([(b, a) for a, b in out], out) if fill else ([], [])
    return closed(out, spares[0]), closed(home, spares[1])


def relay(axis, value, step, fill):
    count = lax.axis_size(axis)
    if count % 2 == 0:
        steps = relay_steps(count, fill)[step]
    else:
        pairs = odd_pairs(count)
        steps = [pairs + [(high, low) for low, high in pairs], [(i, i) for i in range(count)]][step]
    return lax.ppermute(value, axis, steps)


def per_device(object_tiles, probe, phase, measured, offsets, live):
    length = probe.shape[1]
    margin = length // 2
    slots = offsets.shape[0]
    high, wide = object_tiles.shape[2:]
    ext_shape = (2, high + 2 * margin, wide + 2 * margin)
    assert high == 2 * margin
    table = jnp.asarray(dft_table(length))

    def shape(*dims):
        return jax.ShapeDtypeStruct(dims, F32)

    field = shape(2, slots, length, length)
    pieces = (
        *[shape(2, 2, margin, margin)] * 2,
        *[shape(2, high, margin)] * 2,
        shape(2, high + 2 * margin, wide),
    )
    strip = shape(2, margin, wide)
    ext = pltpu.VMEM(ext_shape, F32)
    mid = pltpu.VMEM(field.shape, F32)
    stages = [
        *[pltpu.VMEM((3, length, slots * length), BF16)] * 2,
        *[pltpu.VMEM((3, slots * length, length), BF16)] * 2,
    ]
    params = pltpu.CompilerParams(vmem_limit_bytes=20 * 1024 * 1024)
    small = pltpu.CompilerParams(vmem_limit_bytes=6 * 1024 * 1024)
    cost = pl.CostEstimate(
        flops=2 * 2 * 9 * 2 * slots * length**3, bytes_accessed=8 << 20,
        transcendentals=0,
    )
    call = functools.partial(pl.pallas_call, compiler_params=params)
    call_small = functools.partial(pl.pallas_call, compiler_params=small)
    sides = shape(2, 2, high, margin)
    row_e0, row_o0, row_e1, row_o1, side_e, side_o = call_small(
        edge_kernel,
        out_shape=(*[strip] * 4, sides, sides),
        in_specs=[VMEM],
        out_specs=(VMEM,) * 6,
        name="edges",
    )(object_tiles)
    away = relay("row", row_o1, 0, True)
    halo_e0 = swap("row", row_e0, False)
    halo_o0 = swap("row", row_o0, True)
    halo_e1 = swap("row", row_e1, False)
    side_e = swap("col", side_e, False)
    side_o = swap("col", side_o, True)
    halo_o1 = relay("row", away, 1, True)
    slots_at, kernel, left, probe = call_small(
        turn_kernel,
        out_shape=(
            shape(8 * pl.cdiv(2 * slots + 1, 8), 128),
            shape(2, length, length),
            jax.ShapeDtypeStruct(table.shape, BF16),
            shape(*probe.shape),
        ),
        in_specs=[SMEM] * 2 + [VMEM] * 3,
        out_specs=(VMEM,) * 4,
        name="turn",
    )(offsets, live, phase, table, probe)

    corners = []
    for which, halo in enumerate(((halo_e0, halo_o0), (halo_e1, halo_o1))):
        to_even, to_odd = call_small(
            cut_kernel,
            out_shape=(shape(2, 2, margin, margin),) * 2,
            in_specs=[VMEM, VMEM],
            out_specs=(VMEM, VMEM),
            name=f"cut_{which}",
        )(*halo)
        corners.append((swap("col", to_even, False), swap("col", to_odd, True)))
    near = call(
        near_kernel,
        out_shape=field,
        in_specs=[VMEM] * 11,
        out_specs=VMEM,
        scratch_shapes=[ext, mid, *stages],
        cost_estimate=cost,
        name="near",
    )(
        slots_at, object_tiles, halo_e0, halo_o0, side_e, side_o, *corners[0], probe, kernel,
        left,
    )
    g_near, corner_e, corner_o, one_e, one_o, middle_one = call(
        exit_kernel,
        out_shape=(field, *pieces),
        in_specs=[VMEM] * 11,
        out_specs=(VMEM,) * 6,
        scratch_shapes=[ext, ext, mid, mid, *stages],
        cost_estimate=cost,
        name="exit",
    )(
        slots_at, object_tiles, halo_e1, halo_o1, side_e, side_o, *corners[1], near,
        measured, left,
    )

    def outer_rows(name, odd, middle, corner_e, corner_o):
        return call_small(
            corner_kernel,
            out_shape=(strip, *odd),
            in_specs=[VMEM] * 3,
            out_specs=(VMEM,) * (1 + len(odd)),
            name=name,
        )(middle, corner_e, corner_o)

    corner_e = swap("col", corner_e, False)
    corner_o = swap("col", corner_o, True)
    zero_e, zero_o, side_e, side_o, middle_zero = call(
        first_kernel,
        out_shape=(*pieces[:2], sides, sides, pieces[4]),
        in_specs=[VMEM] * 7,
        out_specs=(VMEM,) * 5,
        scratch_shapes=[ext, mid, *stages],
        cost_estimate=cost,
        name="first",
    )(slots_at, g_near, probe, kernel, left, one_e, one_o)
    rows_e1, rows_o1 = outer_rows("fold_one", (strip,), middle_one, corner_e, corner_o)
    rows_e1 = swap("row", rows_e1, False)
    rows_o1 = [swap("row", rows_o1, True)]
    zero_e = swap("col", zero_e, False)
    zero_o = swap("col", zero_o, True)
    rows_e0, direct, away = outer_rows(
        "fold_zero", (shape(1, margin, wide),) * 2, middle_zero, zero_e, zero_o
    )
    away = relay("row", away, 0, False)
    rows_e0 = swap("row", rows_e0, False)
    direct = swap("row", direct, True)
    rows_o0 = [direct, relay("row", away, 1, False)]
    side_e = swap("col", side_e, False)
    side_o = swap("col", side_o, True)
    whole = shape(*object_tiles.shape)
    outs = ()
    for given, steps in (
        ((middle_one, rows_e1, *rows_o1), ((1, 0, 0, [1]), (1, 1, 0, [2]))),
        ((middle_zero, rows_e0), ((0, 0, 0, [1]),)),
        ((middle_zero, *rows_o0), ((0, 1, 0, [1, 2]),)),
    ):
        rows = pltpu.VMEM((len(steps), 2, margin, wide), F32)
        outs = pl.pallas_call(
            functools.partial(final_kernel, steps),
            out_shape=(whole, whole),
            in_specs=[VMEM] * (3 + len(given)) + [ANY] * len(outs),
            out_specs=(ANY, ANY),
            scratch_shapes=[rows, rows, pltpu.SemaphoreType.DMA((len(steps), 2, 2))],
            input_output_aliases={3 + len(given): 0, 4 + len(given): 1} if outs else {},
            compiler_params=small,
        )(object_tiles, side_e, side_o, *given, *outs)
    return tuple(outs)


def solution(mesh):
    return jax.shard_map(
        per_device,
        mesh=mesh,
        in_specs=(
            P(None, None, "row", "col"),
            P(),
            P(),
            P(("row", "col"), None, None),
            P(("row", "col"), None),
            P("row", "col"),
        ),
        out_specs=(P(None, None, "row", "col"), P(None, None, "row", "col")),
        check_vma=False,
    )
```

```python
import functools
import math

import jax
import jax.numpy as jnp
import numpy as np
from jax import lax
from jax.experimental import pallas as pl
from jax.experimental.pallas import tpu as pltpu
from jax.sharding import PartitionSpec as P


step_size = 0.5


F32 = jnp.float32
BF16 = jnp.bfloat16
VMEM = pl.BlockSpec(memory_space=pltpu.VMEM)
SMEM = pl.BlockSpec(memory_space=pltpu.SMEM)
ANY = pl.BlockSpec(memory_space=pl.ANY)


def split(value):
    high = value.astype(BF16)
    return high, (value - high.astype(F32)).astype(BF16)


def dft_table(length):
    index = np.arange(length)
    angles = (index[:, None] * index[None, :] % length) * (2.0 * math.pi / length)
    cosine, sine = (np.cos(angles) / math.sqrt(length), np.sin(angles) / math.sqrt(length))
    table = np.stack([cosine, cosine + sine, cosine - sine])
    high = table.astype(np.float32).astype(BF16)
    low = (table - high.astype(np.float64)).astype(np.float32).astype(BF16)
    return np.stack([high, low])


def spread(high, low, place, a, b):
    for form, value in enumerate((a + b, a, b)):
        high[(form, *place)], low[(form, *place)] = split(value)


def join(one, two, three):
    return one - three, one - two


def transform(conj, load, store, table, scratch):
    xh, xl, zh, zl = scratch
    length = xh.shape[1]
    slots = xh.shape[2] // length
    order = (1, 0) if conj else (0, 1)
    for slot in range(slots):
        parts = load(slot)
        cols = pl.ds(slot * length, length)
        spread(xh, xl, (slice(None), cols), parts[order[0]], parts[order[1]])
    products = []
    for form in range(3):
        lhs = jnp.concatenate([table[0, form], table[1, form], table[0, form]], axis=1)
        rhs = jnp.concatenate([xh[form], xh[form], xl[form]], axis=0)
        products.append(jnp.dot(lhs, rhs, preferred_element_type=F32))
    z = join(*products)
    for slot in range(slots):
        at = slice(slot * length, (slot + 1) * length)
        spread(zh, zl, (pl.ds(slot * length, length), slice(None)), z[0][:, at], z[1][:, at])
    for slot in range(slots):
        rows = pl.ds(slot * length, length)
        products = []
        for form in range(3):
            lhs = jnp.concatenate([zh[form, rows], zl[form, rows], zh[form, rows]], axis=1)
            rhs = jnp.concatenate([table[0, form], table[0, form], table[1, form]], axis=0)
            products.append(jnp.dot(lhs, rhs, preferred_element_type=F32))
        both = join(*products)
        store(slot, both[order[0]], both[order[1]])


def gather_slice(which, pieces, ext):
    tile, rows, sides, corners = pieces[0], pieces[1:3], pieces[3:5], pieces[5:7]
    margin = rows[0].shape[1]
    places = places_of(margin, *tile.shape[2:])
    inner_rows, inner_cols = pl.ds(margin, tile.shape[2]), pl.ds(margin, tile.shape[3])
    outer_rows, outer_cols = halves(places, 0, margin), halves(places, 2, margin)
    for part in range(2):
        ext[part, inner_rows, inner_cols] = tile[which, part]
        for k in range(2):
            ext[part, outer_rows[k], inner_cols] = rows[k][part]
            ext[part, inner_rows, outer_cols[k]] = sides[k][which, part]
            for j in range(2):
                ext[part, outer_rows[j], outer_cols[k]] = corners[k][j, part]


def places_of(margin, high, wide):
    row_at, col_at = lax.axis_index("row"), lax.axis_index("col")
    row_e = jnp.where(row_at % 2 == 0, margin + high, 0)
    col_e = jnp.where(col_at % 2 == 0, margin + wide, 0)
    partnered = []
    for axis, at in (("row", row_at), ("col", col_at)):
        last = lax.axis_size(axis) - 1
        partnered.append((at > 0) & ((at < last) | (last % 2 == 0)))
    return row_e, margin + high - row_e, col_e, margin + wide - col_e, *partnered


def halves(places, first, margin):
    return [pl.ds(pl.multiple_of(places[first + k], 128), margin) for k in range(2)]


def inner_halves(places, first, margin):
    at = [jnp.maximum(places[first + k] - 2 * margin, 0) for k in range(2)]
    return [pl.ds(pl.multiple_of(start, 128), margin) for start in at]


def kept(value, odd, partnered):
    return jnp.where(partnered, value, 0.0) if odd else value


def hand_out(gext, corners, sides, middle):
    margin = corners[0].shape[2]
    places = places_of(margin, sides[0].shape[1], middle.shape[2])
    inner_rows, inner_cols = pl.ds(margin, sides[0].shape[1]), pl.ds(margin, middle.shape[2])
    outer_rows, outer_cols = halves(places, 0, margin), halves(places, 2, margin)
    for part in range(2):
        for k in range(2):
            for j in range(2):
                corners[k][j, part] = kept(gext[part, outer_rows[j], outer_cols[k]], k, places[5])
            sides[k][part] = kept(gext[part, inner_rows, outer_cols[k]], k, places[5])
        middle[part] = gext[part, :, inner_cols]


def scalar(slots_at, index):
    return jnp.max(slots_at[pl.ds(index, 1), :]).astype(jnp.int32)


def place(slots_at, slot, shape, length):
    spans, shifts = ([], [])
    for axis, tile in ((0, 8), (1, 128)):
        at = scalar(slots_at, 2 * slot + axis)
        base = jnp.minimum(at // tile, (shape[axis + 1] - length) // tile - 1)
        spans.append(pl.ds(pl.multiple_of(base * tile, tile), length + tile))
        shifts.append(at - base * tile)
    return spans, shifts


def window(ext, slots_at, slot, length):
    (rows, cols), (down, along) = place(slots_at, slot, ext.shape, length)
    groups = length // 8
    sublane = lax.broadcasted_iota(jnp.int32, (1, 8, 1), 1) < 8 - down
    lane = lax.broadcasted_iota(jnp.int32, (1, 128), 1) < 128 - along
    parts = []
    for part in range(2):
        tall = ext[part, rows, cols].reshape(groups + 1, 8, length + 128)
        tall = pltpu.roll(tall, lax.rem(8 - down, 8), axis=1)
        flat = jnp.where(sublane, tall[:-1], tall[1:]).reshape(length, length + 128)
        turned = [
            pltpu.roll(flat[:, at : at + 128], lax.rem(128 - along, 128), axis=1)
            for at in range(0, length + 128, 128)
        ]
        pieces = [jnp.where(lane, *pair) for pair in zip(turned[:-1], turned[1:])]
        parts.append(jnp.concatenate(pieces, axis=1))
    return parts


def scatter(gext, slots_at, slot, grads):
    length = grads[0].shape[0]
    (rows, cols), (down, along) = place(slots_at, slot, gext.shape, length)
    groups = length // 8
    sublane = lax.broadcasted_iota(jnp.int32, (1, 8, 1), 1) >= down
    lane = lax.broadcasted_iota(jnp.int32, (1, 128), 1) >= along
    for part in range(2):
        turned = [
            pltpu.roll(grads[part][:, at : at + 128], lax.rem(along, 128), axis=1)
            for at in range(0, length, 128)
        ]
        none = jnp.zeros((length, 128), F32)
        pieces = [jnp.where(lane, *pair) for pair in zip([*turned, none], [none, *turned])]
        flat = jnp.concatenate(pieces, axis=1).reshape(groups, 8, length + 128)
        flat = pltpu.roll(flat, lax.rem(down, 8), axis=1)
        none = jnp.zeros((1, 8, length + 128), F32)
        after, before = (jnp.concatenate(pair, axis=0) for pair in ((flat, none), (none, flat)))
        tall = jnp.where(sublane, after, before).reshape(length + 8, length + 128)
        gext[part, rows, cols] += tall


def multiply(a, b):
    return a[0] * b[0] - a[1] * b[1], a[0] * b[1] + a[1] * b[0]


def multiply_conj(a, b):
    return a[0] * b[0] + a[1] * b[1], a[0] * b[1] - a[1] * b[0]


def put(ref, slot, re, im):
    ref[0, slot] = re
    ref[1, slot] = im


def near_kernel(
    slots_at, tile, row_e, row_o, side_e, side_o, corner_e, corner_o, probe, kernel, left, near,
    ext, mid, xh, xl, zh, zl,
):
    scratch = (xh, xl, zh, zl)
    length = probe.shape[1]
    pieces = (tile, row_e, row_o, side_e, side_o, corner_e, corner_o)
    gather_slice(0, pieces, ext)

    def first(slot):
        return multiply(probe, window(ext, slots_at, slot, length))

    def moved(slot, re, im):
        put(mid, slot, *multiply((re, im), kernel))

    transform(False, first, moved, left, scratch)
    transform(
        True, lambda slot: (mid[0, slot], mid[1, slot]), functools.partial(put, near),
        left, scratch,
    )


def exit_kernel(
    slots_at, tile, row_e, row_o, side_e, side_o, corner_e, corner_o, near, measured, left,
    g_near, out_ce, out_co, out_se, out_so, middle, gext, ext, mid, cut, xh, xl,
    zh, zl,
):
    scratch = (xh, xl, zh, zl)
    length = near.shape[2]
    pieces = (tile, row_e, row_o, side_e, side_o, corner_e, corner_o)
    gather_slice(1, pieces, ext)
    gext[...] = jnp.zeros(gext.shape, F32)

    def exiting(slot):
        put(cut, slot, *window(ext, slots_at, slot, length))
        return multiply((near[0, slot], near[1, slot]), (cut[0, slot], cut[1, slot]))

    def residual(slot, re, im):
        weight = jnp.where(slot < scalar(slots_at, 2 * near.shape[1]), 1.0, 0.0).astype(F32)
        factor = weight * (re * re + im * im - measured[slot])
        put(mid, slot, factor * re, factor * im)

    def back(slot, re, im):
        put(g_near, slot, *multiply_conj((cut[0, slot], cut[1, slot]), (re, im)))
        scatter(gext, slots_at, slot, multiply_conj((near[0, slot], near[1, slot]), (re, im)))

    transform(False, exiting, residual, left, scratch)
    transform(True, lambda slot: (mid[0, slot], mid[1, slot]), back, left, scratch)
    hand_out(gext, (out_ce, out_co), (out_se, out_so), middle)


def first_kernel(
    slots_at, g_near, probe, kernel, left, one_se, one_so, out_ce, out_co, out_se,
    out_so, middle, gext, mid, xh, xl, zh, zl,
):
    scratch = (xh, xl, zh, zl)
    gext[...] = jnp.zeros(gext.shape, F32)

    def moved(slot, re, im):
        put(mid, slot, *multiply_conj(kernel, (re, im)))

    def back(slot, re, im):
        scatter(gext, slots_at, slot, multiply_conj(probe, (re, im)))

    transform(
        False, lambda slot: (g_near[0, slot], g_near[1, slot]), moved, left, scratch
    )
    transform(True, lambda slot: (mid[0, slot], mid[1, slot]), back, left, scratch)
    hand_out(gext, (out_ce, out_co), (out_se.at[0], out_so.at[0]), middle)
    out_se[1] = one_se[...]
    out_so[1] = one_so[...]


def corner_kernel(middle, corner_e, corner_o, strip_e, *strips_o):
    corners, margin = (corner_e, corner_o), corner_e.shape[2]
    places = places_of(margin, middle.shape[1] - 2 * margin, middle.shape[2])
    rows, cols = halves(places, 0, margin), inner_halves(places, 2, margin)
    for part in range(2):
        for strip, at in ((strip_e.at[part], rows[0]), (half(strips_o, part), rows[1])):
            strip[...] = middle[part, at, :]
            for k in range(2):
                strip[:, cols[k]] += corners[k][int(at is rows[1]), part]
    for strip in strips_o:
        strip[...] = kept(strip[...], 1, places[4])


def half(strips, part):
    return strips[part].at[0] if len(strips) == 2 else strips[0].at[part]


def final_kernel(steps, tile, side_e, side_o, *refs):
    after, grad, new_after, new_grad, sems = refs[-5:]
    margin = side_e.shape[3]
    places = places_of(margin, *tile.shape[2:])
    rows, cols = inner_halves(places, 0, margin), inner_halves(places, 2, margin)
    copies = []
    for index, (which, side, middle, arrived) in enumerate(steps):
        arrived = [refs[at] for at in arrived]
        outer = pl.ds(pl.multiple_of(rows[side].start + margin, 128), margin)
        for part in range(2):
            new = new_grad.at[index, part]
            new[...] = refs[middle][part, outer, :] + half(arrived, part)[...]
            for k in range(2):
                new[:, cols[k]] += (side_e, side_o)[k][which, part, rows[side], :]
            stepped = tile[which, part, rows[side], :] - step_size * new[...]
            new_after[index, part] = stepped
            for at, (source, out) in enumerate(((new_after, after), (new_grad, grad))):
                copy = pltpu.make_async_copy(
                    source.at[index, part], out.at[which, part, rows[side], :],
                    sems.at[index, part, at],
                )
                copy.start()
                copies.append(copy)
    for copy in copies:
        copy.wait()


def edge_kernel(tile, row_e0, row_o0, row_e1, row_o1, side_e, side_o):
    margin = row_e0.shape[1]
    places = places_of(margin, *tile.shape[2:])
    rows, cols = inner_halves(places, 0, margin), inner_halves(places, 2, margin)
    for which, outs in enumerate(((row_e0, row_o0), (row_e1, row_o1))):
        for part in range(2):
            for k in range(2):
                outs[k][part] = kept(tile[which, part, rows[k], :], k, places[4])
                side = kept(tile[which, part, :, cols[k]], k, places[5])
                (side_e, side_o)[k][which, part] = side


def cut_kernel(halo_e, halo_o, to_even, to_odd):
    margin = to_even.shape[2]
    places = places_of(margin, 0, halo_e.shape[2])
    cols = inner_halves(places, 2, margin)
    for j, halo in enumerate((halo_e, halo_o)):
        for part in range(2):
            to_even[j, part] = halo[part, :, cols[0]]
            to_odd[j, part] = kept(halo[part, :, cols[1]], 1, places[5])


def turn_kernel(offsets, live, phase, table, light, slots_at, kernel, left, probe):
    count = offsets.shape[0]
    scalars = [offsets[slot, axis] for slot in range(count) for axis in range(2)] + [live[0, 0]]
    row = lax.broadcasted_iota(jnp.int32, slots_at.shape, 0)
    total = jnp.zeros(slots_at.shape, jnp.int32)
    for index, scalar in enumerate(scalars):
        total = jnp.where(row == index, scalar, total)
    slots_at[...] = total.astype(F32)
    left[...] = table[...]
    probe[...] = light[...]
    kernel[0] = jnp.cos(phase[...])
    kernel[1] = jnp.sin(phase[...])


def even_pairs(count):
    return [(low, low + 1) for low in range(0, count - 1, 2)]


def odd_pairs(count):
    return [(low, low + 1) for low in range(1, count - 1, 2)]


def lonely(count):
    paired = {at for pair in odd_pairs(count) for at in pair}
    return [at for at in range(count) if at not in paired]


def swap(axis, value, odd):
    rows, cols = lax.axis_size("row"), lax.axis_size("col")
    pairs = []
    if axis == "row":
        for low, high in odd_pairs(rows) if odd else even_pairs(rows):
            pairs += [((low, col), (high, col)) for col in range(cols)]
        for row in lonely(rows) if odd else ():
            pairs += [((row, low), (row, high)) for low, high in even_pairs(cols)]
    else:
        for low, high in odd_pairs(cols) if odd else even_pairs(cols):
            pairs += [((row, low), (row, high)) for row in range(rows)]
        step = 2 if rows % 4 == 0 else 1
        across = [row for row in range(rows - step) if row // step % 2 == 0]
        for col in lonely(cols) if odd else ():
            pairs += [((row, col), (row + step, col)) for row in across]
    flat = [tuple(row * cols + col for row, col in pair) for pair in pairs]
    return lax.ppermute(value, ("row", "col"), flat + [(b, a) for a, b in flat])


def closed(steps, spare):
    steps = list(steps)
    for source, target in spare:
        if all(source != a and target != b for a, b in steps):
            steps.append((source, target))
    return steps


def relay_steps(count, fill):
    pairs = odd_pairs(count)
    out = [(low, low + 2) for low, high in pairs] + [(high, high - 2) for low, high in pairs]
    home = [(low + 2, high) for low, high in pairs] + [(high - 2, low) for low, high in pairs]
    spares = ([(b, a) for a, b in out], out) if fill else ([], [])
    return closed(out, spares[0]), closed(home, spares[1])


def relay(axis, value, step, fill):
    count = lax.axis_size(axis)
    if count % 2 == 0:
        steps = relay_steps(count, fill)[step]
    else:
        pairs = odd_pairs(count)
        steps = [pairs + [(high, low) for low, high in pairs], [(i, i) for i in range(count)]][step]
    return lax.ppermute(value, axis, steps)


def per_device(object_tiles, probe, phase, measured, offsets, live):
    length = probe.shape[1]
    margin = length // 2
    slots = offsets.shape[0]
    high, wide = object_tiles.shape[2:]
    ext_shape = (2, high + 2 * margin, wide + 2 * margin)
    assert high == 2 * margin
    table = jnp.asarray(dft_table(length))

    def shape(*dims):
        return jax.ShapeDtypeStruct(dims, F32)

    field = shape(2, slots, length, length)
    pieces = (
        *[shape(2, 2, margin, margin)] * 2,
        *[shape(2, high, margin)] * 2,
        shape(2, high + 2 * margin, wide),
    )
    strip = shape(2, margin, wide)
    ext = pltpu.VMEM(ext_shape, F32)
    mid = pltpu.VMEM(field.shape, F32)
    stages = [
        *[pltpu.VMEM((3, length, slots * length), BF16)] * 2,
        *[pltpu.VMEM((3, slots * length, length), BF16)] * 2,
    ]
    params = pltpu.CompilerParams(vmem_limit_bytes=20 * 1024 * 1024)
    small = pltpu.CompilerParams(vmem_limit_bytes=6 * 1024 * 1024)
    cost = pl.CostEstimate(
        flops=2 * 2 * 9 * 2 * slots * length**3, bytes_accessed=8 << 20,
        transcendentals=0,
    )
    call = functools.partial(pl.pallas_call, compiler_params=params)
    call_small = functools.partial(pl.pallas_call, compiler_params=small)
    sides = shape(2, 2, high, margin)
    row_e0, row_o0, row_e1, row_o1, side_e, side_o = call_small(
        edge_kernel,
        out_shape=(*[strip] * 4, sides, sides),
        in_specs=[VMEM],
        out_specs=(VMEM,) * 6,
        name="edges",
    )(object_tiles)
    away = relay("row", row_o1, 0, True)
    halo_e0 = swap("row", row_e0, False)
    halo_o0 = swap("row", row_o0, True)
    halo_e1 = swap("row", row_e1, False)
    side_e = swap("col", side_e, False)
    side_o = swap("col", side_o, True)
    halo_o1 = relay("row", away, 1, True)
    slots_at, kernel, left, probe = call_small(
        turn_kernel,
        out_shape=(
            shape(8 * pl.cdiv(2 * slots + 1, 8), 128),
            shape(2, length, length),
            jax.ShapeDtypeStruct(table.shape, BF16),
            shape(*probe.shape),
        ),
        in_specs=[SMEM] * 2 + [VMEM] * 3,
        out_specs=(VMEM,) * 4,
        name="turn",
    )(offsets, live, phase, table, probe)

    corners = []
    for which, halo in enumerate(((halo_e0, halo_o0), (halo_e1, halo_o1))):
        to_even, to_odd = call_small(
            cut_kernel,
            out_shape=(shape(2, 2, margin, margin),) * 2,
            in_specs=[VMEM, VMEM],
            out_specs=(VMEM, VMEM),
            name=f"cut_{which}",
        )(*halo)
        corners.append((swap("col", to_even, False), swap("col", to_odd, True)))
    near = call(
        near_kernel,
        out_shape=field,
        in_specs=[VMEM] * 11,
        out_specs=VMEM,
        scratch_shapes=[ext, mid, *stages],
        cost_estimate=cost,
        name="near",
    )(
        slots_at, object_tiles, halo_e0, halo_o0, side_e, side_o, *corners[0], probe, kernel,
        left,
    )
    g_near, corner_e, corner_o, one_e, one_o, middle_one = call(
        exit_kernel,
        out_shape=(field, *pieces),
        in_specs=[VMEM] * 11,
        out_specs=(VMEM,) * 6,
        scratch_shapes=[ext, ext, mid, mid, *stages],
        cost_estimate=cost,
        name="exit",
    )(
        slots_at, object_tiles, halo_e1, halo_o1, side_e, side_o, *corners[1], near,
        measured, left,
    )

    def outer_rows(name, odd, middle, corner_e, corner_o):
        return call_small(
            corner_kernel,
            out_shape=(strip, *odd),
            in_specs=[VMEM] * 3,
            out_specs=(VMEM,) * (1 + len(odd)),
            name=name,
        )(middle, corner_e, corner_o)

    corner_e = swap("col", corner_e, False)
    corner_o = swap("col", corner_o, True)
    zero_e, zero_o, side_e, side_o, middle_zero = call(
        first_kernel,
        out_shape=(*pieces[:2], sides, sides, pieces[4]),
        in_specs=[VMEM] * 7,
        out_specs=(VMEM,) * 5,
        scratch_shapes=[ext, mid, *stages],
        cost_estimate=cost,
        name="first",
    )(slots_at, g_near, probe, kernel, left, one_e, one_o)
    rows_e1, rows_o1 = outer_rows("fold_one", (strip,), middle_one, corner_e, corner_o)
    rows_e1 = swap("row", rows_e1, False)
    rows_o1 = [swap("row", rows_o1, True)]
    zero_e = swap("col", zero_e, False)
    zero_o = swap("col", zero_o, True)
    rows_e0, direct, away = outer_rows(
        "fold_zero", (shape(1, margin, wide),) * 2, middle_zero, zero_e, zero_o
    )
    away = relay("row", away, 0, False)
    rows_e0 = swap("row", rows_e0, False)
    direct = swap("row", direct, True)
    rows_o0 = [direct, relay("row", away, 1, False)]
    side_e = swap("col", side_e, False)
    side_o = swap("col", side_o, True)
    whole = shape(*object_tiles.shape)
    outs = ()
    for given, steps in (
        ((middle_one, rows_e1, *rows_o1), ((1, 0, 0, [1]), (1, 1, 0, [2]))),
        ((middle_zero, rows_e0), ((0, 0, 0, [1]),)),
        ((middle_zero, *rows_o0), ((0, 1, 0, [1, 2]),)),
    ):
        rows = pltpu.VMEM((len(steps), 2, margin, wide), F32)
        outs = pl.pallas_call(
            functools.partial(final_kernel, steps),
            out_shape=(whole, whole),
            in_specs=[VMEM] * (3 + len(given)) + [ANY] * len(outs),
            out_specs=(ANY, ANY),
            scratch_shapes=[rows, rows, pltpu.SemaphoreType.DMA((len(steps), 2, 2))],
            input_output_aliases={3 + len(given): 0, 4 + len(given): 1} if outs else {},
            compiler_params=small,
        )(object_tiles, side_e, side_o, *given, *outs)
    return tuple(outs)


def solution(mesh):
    return jax.shard_map(
        per_device,
        mesh=mesh,
        in_specs=(
            P(None, None, "row", "col"),
            P(),
            P(),
            P(("row", "col"), None, None),
            P(("row", "col"), None),
            P("row", "col"),
        ),
        out_specs=(P(None, None, "row", "col"), P(None, None, "row", "col")),
        check_vma=False,
    )
```

```python
import functools
import math

import jax
import jax.numpy as jnp
import numpy as np
from jax import lax
from jax.experimental import pallas as pl
from jax.experimental.pallas import tpu as pltpu
from jax.sharding import PartitionSpec as P


step_size = 0.5


F32 = jnp.float32
BF16 = jnp.bfloat16
VMEM = pl.BlockSpec(memory_space=pltpu.VMEM)
SMEM = pl.BlockSpec(memory_space=pltpu.SMEM)
ANY = pl.BlockSpec(memory_space=pl.ANY)


def split(value):
    high = value.astype(BF16)
    return high, (value - high.astype(F32)).astype(BF16)


def dft_table(length):
    index = np.arange(length)
    angles = (index[:, None] * index[None, :] % length) * (2.0 * math.pi / length)
    cosine, sine = (np.cos(angles) / math.sqrt(length), np.sin(angles) / math.sqrt(length))
    table = np.stack([cosine, cosine + sine, cosine - sine])
    high = table.astype(np.float32).astype(BF16)
    low = (table - high.astype(np.float64)).astype(np.float32).astype(BF16)
    return np.stack([high, low])


def spread(high, low, place, a, b):
    for form, value in enumerate((a + b, a, b)):
        high[(form, *place)], low[(form, *place)] = split(value)


def join(one, two, three):
    return one - three, one - two


def transform(conj, load, store, table, scratch):
    xh, xl, zh, zl = scratch
    length = xh.shape[1]
    slots = xh.shape[2] // length
    order = (1, 0) if conj else (0, 1)
    for slot in range(slots):
        parts = load(slot)
        cols = pl.ds(slot * length, length)
        spread(xh, xl, (slice(None), cols), parts[order[0]], parts[order[1]])
    products = []
    for form in range(3):
        lhs = jnp.concatenate([table[0, form], table[1, form], table[0, form]], axis=1)
        rhs = jnp.concatenate([xh[form], xh[form], xl[form]], axis=0)
        products.append(jnp.dot(lhs, rhs, preferred_element_type=F32))
    z = join(*products)
    for slot in range(slots):
        at = slice(slot * length, (slot + 1) * length)
        spread(zh, zl, (pl.ds(slot * length, length), slice(None)), z[0][:, at], z[1][:, at])
    for slot in range(slots):
        rows = pl.ds(slot * length, length)
        products = []
        for form in range(3):
            lhs = jnp.concatenate([zh[form, rows], zl[form, rows], zh[form, rows]], axis=1)
            rhs = jnp.concatenate([table[0, form], table[0, form], table[1, form]], axis=0)
            products.append(jnp.dot(lhs, rhs, preferred_element_type=F32))
        both = join(*products)
        store(slot, both[order[0]], both[order[1]])


def gather_slice(which, pieces, ext):
    tile, rows, sides, corners = pieces[0], pieces[1:3], pieces[3:5], pieces[5:7]
    margin = rows[0].shape[1]
    places = places_of(margin, *tile.shape[2:])
    inner_rows, inner_cols = pl.ds(margin, tile.shape[2]), pl.ds(margin, tile.shape[3])
    outer_rows, outer_cols = halves(places, 0, margin), halves(places, 2, margin)
    for part in range(2):
        ext[part, inner_rows, inner_cols] = tile[which, part]
        for k in range(2):
            ext[part, outer_rows[k], inner_cols] = rows[k][part]
            ext[part, inner_rows, outer_cols[k]] = sides[k][which, part]
            for j in range(2):
                ext[part, outer_rows[j], outer_cols[k]] = corners[k][j, part]


def places_of(margin, high, wide):
    row_at, col_at = lax.axis_index("row"), lax.axis_index("col")
    row_e = jnp.where(row_at % 2 == 0, margin + high, 0)
    col_e = jnp.where(col_at % 2 == 0, margin + wide, 0)
    partnered = []
    for axis, at in (("row", row_at), ("col", col_at)):
        last = lax.axis_size(axis) - 1
        partnered.append((at > 0) & ((at < last) | (last % 2 == 0)))
    return row_e, margin + high - row_e, col_e, margin + wide - col_e, *partnered


def halves(places, first, margin):
    return [pl.ds(pl.multiple_of(places[first + k], 128), margin) for k in range(2)]


def inner_halves(places, first, margin):
    at = [jnp.maximum(places[first + k] - 2 * margin, 0) for k in range(2)]
    return [pl.ds(pl.multiple_of(start, 128), margin) for start in at]


def kept(value, odd, partnered):
    return jnp.where(partnered, value, 0.0) if odd else value


def hand_out(gext, corners, sides, middle):
    margin = corners[0].shape[2]
    places = places_of(margin, sides[0].shape[1], middle.shape[2])
    inner_rows, inner_cols = pl.ds(margin, sides[0].shape[1]), pl.ds(margin, middle.shape[2])
    outer_rows, outer_cols = halves(places, 0, margin), halves(places, 2, margin)
    for part in range(2):
        for k in range(2):
            for j in range(2):
                corners[k][j, part] = kept(gext[part, outer_rows[j], outer_cols[k]], k, places[5])
            sides[k][part] = kept(gext[part, inner_rows, outer_cols[k]], k, places[5])
        middle[part] = gext[part, :, inner_cols]


def scalar(slots_at, index):
    return jnp.max(slots_at[pl.ds(index, 1), :]).astype(jnp.int32)


def place(slots_at, slot, shape, length):
    spans, shifts = ([], [])
    for axis, tile in ((0, 8), (1, 128)):
        at = scalar(slots_at, 2 * slot + axis)
        base = jnp.minimum(at // tile, (shape[axis + 1] - length) // tile - 1)
        spans.append(pl.ds(pl.multiple_of(base * tile, tile), length + tile))
        shifts.append(at - base * tile)
    return spans, shifts


def window(ext, slots_at, slot, length):
    (rows, cols), (down, along) = place(slots_at, slot, ext.shape, length)
    groups = length // 8
    sublane = lax.broadcasted_iota(jnp.int32, (1, 8, 1), 1) < 8 - down
    lane = lax.broadcasted_iota(jnp.int32, (1, 128), 1) < 128 - along
    parts = []
    for part in range(2):
        tall = ext[part, rows, cols].reshape(groups + 1, 8, length + 128)
        tall = pltpu.roll(tall, lax.rem(8 - down, 8), axis=1)
        flat = jnp.where(sublane, tall[:-1], tall[1:]).reshape(length, length + 128)
        turned = [
            pltpu.roll(flat[:, at : at + 128], lax.rem(128 - along, 128), axis=1)
            for at in range(0, length + 128, 128)
        ]
        pieces = [jnp.where(lane, *pair) for pair in zip(turned[:-1], turned[1:])]
        parts.append(jnp.concatenate(pieces, axis=1))
    return parts


def scatter(gext, slots_at, slot, grads):
    length = grads[0].shape[0]
    (rows, cols), (down, along) = place(slots_at, slot, gext.shape, length)
    groups = length // 8
    sublane = lax.broadcasted_iota(jnp.int32, (1, 8, 1), 1) >= down
    lane = lax.broadcasted_iota(jnp.int32, (1, 128), 1) >= along
    for part in range(2):
        turned = [
            pltpu.roll(grads[part][:, at : at + 128], lax.rem(along, 128), axis=1)
            for at in range(0, length, 128)
        ]
        none = jnp.zeros((length, 128), F32)
        pieces = [jnp.where(lane, *pair) for pair in zip([*turned, none], [none, *turned])]
        flat = jnp.concatenate(pieces, axis=1).reshape(groups, 8, length + 128)
        flat = pltpu.roll(flat, lax.rem(down, 8), axis=1)
        none = jnp.zeros((1, 8, length + 128), F32)
        after, before = (jnp.concatenate(pair, axis=0) for pair in ((flat, none), (none, flat)))
        tall = jnp.where(sublane, after, before).reshape(length + 8, length + 128)
        gext[part, rows, cols] += tall


def multiply(a, b):
    return a[0] * b[0] - a[1] * b[1], a[0] * b[1] + a[1] * b[0]


def multiply_conj(a, b):
    return a[0] * b[0] + a[1] * b[1], a[0] * b[1] - a[1] * b[0]


def put(ref, slot, re, im):
    ref[0, slot] = re
    ref[1, slot] = im


def near_kernel(
    slots_at, tile, row_e, row_o, side_e, side_o, corner_e, corner_o, probe, kernel, left, near,
    ext, mid, xh, xl, zh, zl,
):
    scratch = (xh, xl, zh, zl)
    length = probe.shape[1]
    pieces = (tile, row_e, row_o, side_e, side_o, corner_e, corner_o)
    gather_slice(0, pieces, ext)

    def first(slot):
        return multiply(probe, window(ext, slots_at, slot, length))

    def moved(slot, re, im):
        put(mid, slot, *multiply((re, im), kernel))

    transform(False, first, moved, left, scratch)
    transform(
        True, lambda slot: (mid[0, slot], mid[1, slot]), functools.partial(put, near),
        left, scratch,
    )


def exit_kernel(
    slots_at, tile, row_e, row_o, side_e, side_o, corner_e, corner_o, near, measured, left,
    g_near, out_ce, out_co, out_se, out_so, middle, gext, ext, mid, cut, xh, xl,
    zh, zl,
):
    scratch = (xh, xl, zh, zl)
    length = near.shape[2]
    pieces = (tile, row_e, row_o, side_e, side_o, corner_e, corner_o)
    gather_slice(1, pieces, ext)
    gext[...] = jnp.zeros(gext.shape, F32)

    def exiting(slot):
        put(cut, slot, *window(ext, slots_at, slot, length))
        return multiply((near[0, slot], near[1, slot]), (cut[0, slot], cut[1, slot]))

    def residual(slot, re, im):
        weight = jnp.where(slot < scalar(slots_at, 2 * near.shape[1]), 1.0, 0.0).astype(F32)
        factor = weight * (re * re + im * im - measured[slot])
        put(mid, slot, factor * re, factor * im)

    def back(slot, re, im):
        put(g_near, slot, *multiply_conj((cut[0, slot], cut[1, slot]), (re, im)))
        scatter(gext, slots_at, slot, multiply_conj((near[0, slot], near[1, slot]), (re, im)))

    transform(False, exiting, residual, left, scratch)
    transform(True, lambda slot: (mid[0, slot], mid[1, slot]), back, left, scratch)
    hand_out(gext, (out_ce, out_co), (out_se, out_so), middle)


def first_kernel(
    slots_at, g_near, probe, kernel, left, one_se, one_so, out_ce, out_co, out_se,
    out_so, middle, gext, mid, xh, xl, zh, zl,
):
    scratch = (xh, xl, zh, zl)
    gext[...] = jnp.zeros(gext.shape, F32)

    def moved(slot, re, im):
        put(mid, slot, *multiply_conj(kernel, (re, im)))

    def back(slot, re, im):
        scatter(gext, slots_at, slot, multiply_conj(probe, (re, im)))

    transform(
        False, lambda slot: (g_near[0, slot], g_near[1, slot]), moved, left, scratch
    )
    transform(True, lambda slot: (mid[0, slot], mid[1, slot]), back, left, scratch)
    hand_out(gext, (out_ce, out_co), (out_se.at[0], out_so.at[0]), middle)
    out_se[1] = one_se[...]
    out_so[1] = one_so[...]


def corner_kernel(middle, corner_e, corner_o, strip_e, *strips_o):
    corners, margin = (corner_e, corner_o), corner_e.shape[2]
    places = places_of(margin, middle.shape[1] - 2 * margin, middle.shape[2])
    rows, cols = halves(places, 0, margin), inner_halves(places, 2, margin)
    for part in range(2):
        for strip, at in ((strip_e.at[part], rows[0]), (half(strips_o, part), rows[1])):
            strip[...] = middle[part, at, :]
            for k in range(2):
                strip[:, cols[k]] += corners[k][int(at is rows[1]), part]
    for strip in strips_o:
        strip[...] = kept(strip[...], 1, places[4])


def half(strips, part):
    return strips[part].at[0] if len(strips) == 2 else strips[0].at[part]


def final_kernel(steps, tile, side_e, side_o, *refs):
    after, grad, new_after, new_grad, sems = refs[-5:]
    margin = side_e.shape[3]
    places = places_of(margin, *tile.shape[2:])
    rows, cols = inner_halves(places, 0, margin), inner_halves(places, 2, margin)
    copies = []
    for index, (which, side, middle, arrived) in enumerate(steps):
        arrived = [refs[at] for at in arrived]
        outer = pl.ds(pl.multiple_of(rows[side].start + margin, 128), margin)
        for part in range(2):
            new = new_grad.at[index, part]
            new[...] = refs[middle][part, outer, :] + half(arrived, part)[...]
            for k in range(2):
                new[:, cols[k]] += (side_e, side_o)[k][which, part, rows[side], :]
            stepped = tile[which, part, rows[side], :] - step_size * new[...]
            new_after[index, part] = stepped
            for at, (source, out) in enumerate(((new_after, after), (new_grad, grad))):
                copy = pltpu.make_async_copy(
                    source.at[index, part], out.at[which, part, rows[side], :],
                    sems.at[index, part, at],
                )
                copy.start()
                copies.append(copy)
    for copy in copies:
        copy.wait()


def edge_kernel(tile, row_e0, row_o0, row_e1, row_o1, side_e, side_o):
    margin = row_e0.shape[1]
    places = places_of(margin, *tile.shape[2:])
    rows, cols = inner_halves(places, 0, margin), inner_halves(places, 2, margin)
    for which, outs in enumerate(((row_e0, row_o0), (row_e1, row_o1))):
        for part in range(2):
            for k in range(2):
                outs[k][part] = kept(tile[which, part, rows[k], :], k, places[4])
                side = kept(tile[which, part, :, cols[k]], k, places[5])
                (side_e, side_o)[k][which, part] = side


def cut_kernel(halo_e, halo_o, to_even, to_odd):
    margin = to_even.shape[2]
    places = places_of(margin, 0, halo_e.shape[2])
    cols = inner_halves(places, 2, margin)
    for j, halo in enumerate((halo_e, halo_o)):
        for part in range(2):
            to_even[j, part] = halo[part, :, cols[0]]
            to_odd[j, part] = kept(halo[part, :, cols[1]], 1, places[5])


def turn_kernel(offsets, live, phase, table, light, slots_at, kernel, left, probe):
    count = offsets.shape[0]
    scalars = [offsets[slot, axis] for slot in range(count) for axis in range(2)] + [live[0, 0]]
    row = lax.broadcasted_iota(jnp.int32, slots_at.shape, 0)
    total = jnp.zeros(slots_at.shape, jnp.int32)
    for index, scalar in enumerate(scalars):
        total = jnp.where(row == index, scalar, total)
    slots_at[...] = total.astype(F32)
    left[...] = table[...]
    probe[...] = light[...]
    kernel[0] = jnp.cos(phase[...])
    kernel[1] = jnp.sin(phase[...])


def even_pairs(count):
    return [(low, low + 1) for low in range(0, count - 1, 2)]


def odd_pairs(count):
    return [(low, low + 1) for low in range(1, count - 1, 2)]


def lonely(count):
    paired = {at for pair in odd_pairs(count) for at in pair}
    return [at for at in range(count) if at not in paired]


def swap(axis, value, odd, fill=True):
    rows, cols = lax.axis_size("row"), lax.axis_size("col")
    pairs = []
    if axis == "row":
        for low, high in odd_pairs(rows) if odd else even_pairs(rows):
            pairs += [((low, col), (high, col)) for col in range(cols)]
        for row in lonely(rows) if odd and fill else ():
            pairs += [((row, low), (row, high)) for low, high in even_pairs(cols)]
    else:
        for low, high in odd_pairs(cols) if odd else even_pairs(cols):
            pairs += [((row, low), (row, high)) for row in range(rows)]
        step = 2 if rows % 4 == 0 else 1
        across = [row for row in range(rows - step) if row // step % 2 == 0]
        for col in lonely(cols) if odd and fill else ():
            pairs += [((row, col), (row + step, col)) for row in across]
    flat = [tuple(row * cols + col for row, col in pair) for pair in pairs]
    return lax.ppermute(value, ("row", "col"), flat + [(b, a) for a, b in flat])


def closed(steps, spare):
    steps = list(steps)
    for source, target in spare:
        if all(source != a and target != b for a, b in steps):
            steps.append((source, target))
    return steps


def relay_steps(count, fill):
    pairs = odd_pairs(count)
    out = [(low, low + 2) for low, high in pairs] + [(high, high - 2) for low, high in pairs]
    home = [(low + 2, high) for low, high in pairs] + [(high - 2, low) for low, high in pairs]
    spares = ([(b, a) for a, b in out], out) if fill else ([], [])
    return closed(out, spares[0]), closed(home, spares[1])


def relay(axis, value, step, fill):
    count = lax.axis_size(axis)
    if count % 2 == 0:
        steps = relay_steps(count, fill)[step]
    else:
        pairs = odd_pairs(count)
        steps = [pairs + [(high, low) for low, high in pairs], [(i, i) for i in range(count)]][step]
    return lax.ppermute(value, axis, steps)


def per_device(object_tiles, probe, phase, measured, offsets, live):
    length = probe.shape[1]
    margin = length // 2
    slots = offsets.shape[0]
    high, wide = object_tiles.shape[2:]
    ext_shape = (2, high + 2 * margin, wide + 2 * margin)
    assert high == 2 * margin
    table = jnp.asarray(dft_table(length))

    def shape(*dims):
        return jax.ShapeDtypeStruct(dims, F32)

    field = shape(2, slots, length, length)
    pieces = (
        *[shape(2, 2, margin, margin)] * 2,
        *[shape(2, high, margin)] * 2,
        shape(2, high + 2 * margin, wide),
    )
    strip = shape(2, margin, wide)
    ext = pltpu.VMEM(ext_shape, F32)
    mid = pltpu.VMEM(field.shape, F32)
    stages = [
        *[pltpu.VMEM((3, length, slots * length), BF16)] * 2,
        *[pltpu.VMEM((3, slots * length, length), BF16)] * 2,
    ]
    params = pltpu.CompilerParams(vmem_limit_bytes=20 * 1024 * 1024)
    small = pltpu.CompilerParams(vmem_limit_bytes=6 * 1024 * 1024)
    cost = pl.CostEstimate(
        flops=2 * 2 * 9 * 2 * slots * length**3, bytes_accessed=8 << 20,
        transcendentals=0,
    )
    call = functools.partial(pl.pallas_call, compiler_params=params)
    call_small = functools.partial(pl.pallas_call, compiler_params=small)
    sides = shape(2, 2, high, margin)
    row_e0, row_o0, row_e1, row_o1, side_e, side_o = call_small(
        edge_kernel,
        out_shape=(*[strip] * 4, sides, sides),
        in_specs=[VMEM],
        out_specs=(VMEM,) * 6,
        name="edges",
    )(object_tiles)
    away = relay("row", row_o1, 0, True)
    halo_e0 = swap("row", row_e0, False)
    halo_o0 = swap("row", row_o0, True)
    halo_e1 = swap("row", row_e1, False)
    side_e = swap("col", side_e, False)
    side_o = swap("col", side_o, True)
    halo_o1 = relay("row", away, 1, True)
    slots_at, kernel, left, probe = call_small(
        turn_kernel,
        out_shape=(
            shape(8 * pl.cdiv(2 * slots + 1, 8), 128),
            shape(2, length, length),
            jax.ShapeDtypeStruct(table.shape, BF16),
            shape(*probe.shape),
        ),
        in_specs=[SMEM] * 2 + [VMEM] * 3,
        out_specs=(VMEM,) * 4,
        name="turn",
    )(offsets, live, phase, table, probe)

    corners = []
    for which, halo in enumerate(((halo_e0, halo_o0), (halo_e1, halo_o1))):
        to_even, to_odd = call_small(
            cut_kernel,
            out_shape=(shape(2, 2, margin, margin),) * 2,
            in_specs=[VMEM, VMEM],
            out_specs=(VMEM, VMEM),
            name=f"cut_{which}",
        )(*halo)
        corners.append((swap("col", to_even, False), swap("col", to_odd, True)))
    near = call(
        near_kernel,
        out_shape=field,
        in_specs=[VMEM] * 11,
        out_specs=VMEM,
        scratch_shapes=[ext, mid, *stages],
        cost_estimate=cost,
        name="near",
    )(
        slots_at, object_tiles, halo_e0, halo_o0, side_e, side_o, *corners[0], probe, kernel,
        left,
    )
    g_near, corner_e, corner_o, one_e, one_o, middle_one = call(
        exit_kernel,
        out_shape=(field, *pieces),
        in_specs=[VMEM] * 11,
        out_specs=(VMEM,) * 6,
        scratch_shapes=[ext, ext, mid, mid, *stages],
        cost_estimate=cost,
        name="exit",
    )(
        slots_at, object_tiles, halo_e1, halo_o1, side_e, side_o, *corners[1], near,
        measured, left,
    )

    def outer_rows(name, odd, middle, corner_e, corner_o):
        return call_small(
            corner_kernel,
            out_shape=(strip, *odd),
            in_specs=[VMEM] * 3,
            out_specs=(VMEM,) * (1 + len(odd)),
            name=name,
        )(middle, corner_e, corner_o)

    corner_e = swap("col", corner_e, False)
    corner_o = swap("col", corner_o, True)
    zero_e, zero_o, side_e, side_o, middle_zero = call(
        first_kernel,
        out_shape=(*pieces[:2], sides, sides, pieces[4]),
        in_specs=[VMEM] * 7,
        out_specs=(VMEM,) * 5,
        scratch_shapes=[ext, mid, *stages],
        cost_estimate=cost,
        name="first",
    )(slots_at, g_near, probe, kernel, left, one_e, one_o)
    rows_e1, rows_o1 = outer_rows("fold_one", (strip,), middle_one, corner_e, corner_o)
    rows_e1 = swap("row", rows_e1, False)
    rows_o1 = [swap("row", rows_o1, True)]
    zero_e = swap("col", zero_e, False)
    zero_o = swap("col", zero_o, True)
    rows_e0, direct, away = outer_rows(
        "fold_zero", (shape(1, margin, wide),) * 2, middle_zero, zero_e, zero_o
    )
    away = relay("row", away, 0, False)
    rows_e0 = swap("row", rows_e0, False)
    direct = swap("row", direct, True)
    rows_o0 = [direct, relay("row", away, 1, False)]
    side_e = swap("col", side_e, False)
    side_o = swap("col", side_o, True, False)
    whole = shape(*object_tiles.shape)
    outs = ()
    for given, steps in (
        ((middle_one, rows_e1, *rows_o1), ((1, 0, 0, [1]), (1, 1, 0, [2]))),
        ((middle_zero, rows_e0), ((0, 0, 0, [1]),)),
        ((middle_zero, *rows_o0), ((0, 1, 0, [1, 2]),)),
    ):
        rows = pltpu.VMEM((len(steps), 2, margin, wide), F32)
        outs = pl.pallas_call(
            functools.partial(final_kernel, steps),
            out_shape=(whole, whole),
            in_specs=[VMEM] * (3 + len(given)) + [ANY] * len(outs),
            out_specs=(ANY, ANY),
            scratch_shapes=[rows, rows, pltpu.SemaphoreType.DMA((len(steps), 2, 2))],
            input_output_aliases={3 + len(given): 0, 4 + len(given): 1} if outs else {},
            compiler_params=small,
        )(object_tiles, side_e, side_o, *given, *outs)
    return tuple(outs)


def solution(mesh):
    return jax.shard_map(
        per_device,
        mesh=mesh,
        in_specs=(
            P(None, None, "row", "col"),
            P(),
            P(),
            P(("row", "col"), None, None),
            P(("row", "col"), None),
            P("row", "col"),
        ),
        out_specs=(P(None, None, "row", "col"), P(None, None, "row", "col")),
        check_vma=False,
    )
```
